128 devices in a mesh: batch: 1, graph: 128 (over z, y, x, core).
Axes of the slice: x: 4, y: 4, z: 4, core: 2. Of those that a mesh axis runs over, the one named last changes fastest.
Arguments:
- grid_in: float32 [65536, 267], P(('batch', 'graph'))
- mesh_in: float32 [131072, 3], P(('batch', 'graph'))
- edge_in: float32 [1048576, 4], P(('batch', 'graph'))
- edge_src: int32 [1048576], P(('batch', 'graph'))
- edge_dst: int32 [1048576], P(('batch', 'graph'))
- edge_mask: int32 [1048576], P(('batch', 'graph'))
- grid_w1: bfloat16 [267, 512], replicated
- grid_w2: bfloat16 [512, 512], replicated
- grid_vec: float32 [4, 512], replicated
- mesh_w1: bfloat16 [3, 512], replicated
- mesh_w2: bfloat16 [512, 512], replicated
- mesh_vec: float32 [4, 512], replicated
- embed_w1: bfloat16 [4, 512], replicated
- embed_w2: bfloat16 [512, 512], replicated
- embed_vec: float32 [4, 512], replicated
- edge_w1: bfloat16 [1536, 512], replicated
- edge_w2: bfloat16 [512, 512], replicated
- edge_vec: float32 [4, 512], replicated
- node_w1: bfloat16 [1024, 512], replicated
- node_w2: bfloat16 [512, 512], replicated
- node_vec: float32 [4, 512], replicated
- post_w1: bfloat16 [512, 512], replicated
- post_w2: bfloat16 [512, 512], replicated
- post_vec: float32 [4, 512], replicated
- cot_mesh: bfloat16 [131072, 512], P(('batch', 'graph'))
- cot_grid: bfloat16 [65536, 512], P(('batch', 'graph'))
Outputs:
- output 1: bfloat16 [131072, 512], P(('batch', 'graph'))
- output 2: bfloat16 [65536, 512], P(('batch', 'graph'))
- output 3: float32 [65536, 267], P(('batch', 'graph'))
- output 4: float32 [1536, 512], P(('batch', 'graph'))
- output 5: float32 [512, 512], P(('batch', 'graph'))
All inputs are finite; a program needn't handle non-finite values.
Results may differ from the reference program's by a relative error of at most 0.0100959.
Values are sent between devices in bfloat16 or wider.
A program may use at most 1 GiB of HBM per device.

```python
import jax
import jax.numpy as jnp
from jax import lax

GROUP_SIZE = 128
GRID_DEV = 512
MESH_DEV = 1024
EDGE_DEV = 8192
LATENT = 512
GRID_FEAT = 267
MESH_FEAT = 3
EDGE_FEAT = 4

NORM_EPS = 1e-5
HALO_ROWS = GRID_DEV // 4
GRID_ROWS = GROUP_SIZE * GRID_DEV
MESH_ROWS = GROUP_SIZE * MESH_DEV
EDGE_ROWS = GROUP_SIZE * EDGE_DEV
AGG_SCALE = max(EDGE_DEV // MESH_DEV, 1) ** -0.5


def draw_graph(graph_key):
    sub_keys = jax.random.split(graph_key, 8)
    band_idx = jnp.arange(GROUP_SIZE)[:, None]
    edge_col = jnp.arange(EDGE_DEV)[None, :]
    cut_pct = jax.random.randint(sub_keys[0], (GROUP_SIZE, 1), 20, 61)
    keep_pct = jax.random.randint(sub_keys[1], (GROUP_SIZE, 1), 25, 101)
    roll_pct = jax.random.randint(sub_keys[2], (GROUP_SIZE, EDGE_DEV), 0, 100)
    local_off = jax.random.randint(sub_keys[3], (GROUP_SIZE, EDGE_DEV), 0, GRID_DEV)
    halo_off = jax.random.randint(sub_keys[4], (GROUP_SIZE, EDGE_DEV), 0, HALO_ROWS)
    take_low = (roll_pct < cut_pct // 2) & (band_idx > 0)
    take_high = (roll_pct >= cut_pct // 2) & (roll_pct < cut_pct) & (band_idx < GROUP_SIZE - 1)
    src_ids = jnp.where(take_low, band_idx * GRID_DEV - 1 - halo_off,
                        jnp.where(take_high, (band_idx + 1) * GRID_DEV + halo_off, band_idx * GRID_DEV + local_off))
    low_end = jnp.maximum(band_idx * GRID_DEV - HALO_ROWS, 0)
    high_end = jnp.minimum((band_idx + 1) * GRID_DEV + HALO_ROWS, GRID_ROWS) - 1
    src_ids = jnp.where(edge_col == 0, low_end, jnp.where(edge_col == 1, high_end, src_ids))
    shift_by = jax.random.randint(sub_keys[5], (GROUP_SIZE, 1), 0, MESH_DEV)
    rand_dst = jax.random.randint(sub_keys[6], (GROUP_SIZE, EDGE_DEV), 0, MESH_DEV)
    dst_ids = jnp.where(edge_col < MESH_DEV, (edge_col + shift_by) % MESH_DEV, rand_dst)
    keep_flag = (jax.random.randint(sub_keys[7], (GROUP_SIZE, EDGE_DEV), 0, 100) < keep_pct) | (edge_col < 2)
    return (src_ids.reshape(EDGE_ROWS).astype(jnp.int32),
            dst_ids.reshape(EDGE_ROWS).astype(jnp.int32),
            keep_flag.reshape(EDGE_ROWS).astype(jnp.int32))


def draw_mlp(mlp_key, fan_in, row_scale):
    sub_keys = jax.random.split(mlp_key, 3)
    w_one = jax.random.normal(sub_keys[0], (fan_in, LATENT), jnp.float32) * row_scale * fan_in ** -0.5
    w_two = jax.random.normal(sub_keys[1], (LATENT, LATENT), jnp.float32) * LATENT ** -0.5
    vec_rows = 0.3 * jax.random.normal(sub_keys[2], (4, LATENT), jnp.float32) + jnp.array([[0.0], [0.0], [1.0], [0.0]], jnp.float32)
    return w_one.astype(jnp.bfloat16), w_two.astype(jnp.bfloat16), vec_rows


def setup_inputs(seed: int = 0, part: int = 0) -> dict:
    root_key = jax.random.key(seed)
    part_key = jax.random.fold_in(root_key, part)
    data_keys = jax.random.split(part_key, 8)
    weight_keys = jax.random.split(jax.random.key(seed + 1), 6)
    lat_pos = (jnp.arange(GRID_ROWS, dtype=jnp.float32) + 0.5) / GRID_ROWS
    freq_rows = jax.random.randint(data_keys[0], (GRID_FEAT,), 1, 9).astype(jnp.float32)
    phase_rows = jax.random.uniform(data_keys[1], (GRID_FEAT,), jnp.float32, 0.0, 6.2832)
    grid_in = jax.random.normal(data_keys[2], (GRID_ROWS, GRID_FEAT), jnp.float32) + 1.5 * jnp.cos(
        jnp.pi * lat_pos[:, None] * freq_rows[None, :] + phase_rows[None, :])
    mesh_in = jax.random.normal(data_keys[3], (MESH_ROWS, MESH_FEAT), jnp.float32)
    edge_in = jax.random.normal(data_keys[4], (EDGE_ROWS, EDGE_FEAT), jnp.float32)
    edge_src, edge_dst, edge_mask = draw_graph(data_keys[5])
    cot_mesh = jax.random.normal(data_keys[6], (MESH_ROWS, LATENT), jnp.float32).astype(jnp.bfloat16)
    cot_grid = (0.25 * jax.random.normal(data_keys[7], (GRID_ROWS, LATENT), jnp.float32)).astype(jnp.bfloat16)
    grid_w1, grid_w2, grid_vec = draw_mlp(weight_keys[0], GRID_FEAT, 1.0)
    mesh_w1, mesh_w2, mesh_vec = draw_mlp(weight_keys[1], MESH_FEAT, 1.0)
    embed_w1, embed_w2, embed_vec = draw_mlp(weight_keys[2], EDGE_FEAT, 1.0)
    edge_w1, edge_w2, edge_vec = draw_mlp(weight_keys[3], 3 * LATENT, 1.0)
    node_scale = jnp.concatenate([jnp.ones((LATENT, 1), jnp.float32), jnp.full((LATENT, 1), AGG_SCALE, jnp.float32)], axis=0)
    node_w1, node_w2, node_vec = draw_mlp(weight_keys[4], 2 * LATENT, node_scale)
    post_w1, post_w2, post_vec = draw_mlp(weight_keys[5], LATENT, 1.0)
    return {'grid_in': grid_in, 'mesh_in': mesh_in, 'edge_in': edge_in, 'edge_src': edge_src, 'edge_dst': edge_dst,
            'edge_mask': edge_mask, 'grid_w1': grid_w1, 'grid_w2': grid_w2, 'grid_vec': grid_vec,
            'mesh_w1': mesh_w1, 'mesh_w2': mesh_w2, 'mesh_vec': mesh_vec, 'embed_w1': embed_w1,
            'embed_w2': embed_w2, 'embed_vec': embed_vec, 'edge_w1': edge_w1, 'edge_w2': edge_w2,
            'edge_vec': edge_vec, 'node_w1': node_w1, 'node_w2': node_w2, 'node_vec': node_vec,
            'post_w1': post_w1, 'post_w2': post_w2, 'post_vec': post_vec, 'cot_mesh': cot_mesh,
            'cot_grid': cot_grid}


def mlp_forward(x_in, w_one, w_two, vec_rows):
    pre_one = jnp.dot(x_in, w_one, preferred_element_type=jnp.float32) + vec_rows[0]
    act_bf = jax.nn.silu(pre_one).astype(jnp.bfloat16)
    pre_two = jnp.dot(act_bf, w_two, preferred_element_type=jnp.float32) + vec_rows[1]
    centred = pre_two - jnp.mean(pre_two, axis=-1, keepdims=True)
    inv_std = lax.rsqrt(jnp.mean(centred * centred, axis=-1, keepdims=True) + NORM_EPS)
    normed = centred * inv_std
    return normed * vec_rows[2] + vec_rows[3], (pre_one, act_bf, normed, inv_std)


def mlp_backward(d_out, w_two, vec_rows, saved_acts):
    pre_one, act_bf, normed, inv_std = saved_acts
    d_norm = d_out * vec_rows[2]
    d_two = inv_std * (d_norm - jnp.mean(d_norm, axis=-1, keepdims=True)
                       - normed * jnp.mean(d_norm * normed, axis=-1, keepdims=True))
    g_two = d_two.astype(jnp.bfloat16)
    d_act = jnp.dot(g_two, w_two.T, preferred_element_type=jnp.float32)
    sig_pre = jax.nn.sigmoid(pre_one)
    d_one = d_act * sig_pre * (1.0 + pre_one * (1.0 - sig_pre))
    return d_one.astype(jnp.bfloat16), g_two


def reference(grid_in, mesh_in, edge_in, edge_src, edge_dst, edge_mask, grid_w1, grid_w2, grid_vec,
              mesh_w1, mesh_w2, mesh_vec, embed_w1, embed_w2, embed_vec, edge_w1, edge_w2, edge_vec,
              node_w1, node_w2, node_vec, post_w1, post_w2, post_vec, cot_mesh, cot_grid):
    grid_y, grid_saved = mlp_forward(grid_in.astype(jnp.bfloat16), grid_w1, grid_w2, grid_vec)
    grid_h = grid_y.astype(jnp.bfloat16)
    post_y, post_saved = mlp_forward(grid_h, post_w1, post_w2, post_vec)
    grid_out = (grid_h.astype(jnp.float32) + post_y).astype(jnp.bfloat16)
    blocks = (mesh_in.reshape(GROUP_SIZE, MESH_DEV, MESH_FEAT),
              edge_in.reshape(GROUP_SIZE, EDGE_DEV, EDGE_FEAT),
              edge_src.reshape(GROUP_SIZE, EDGE_DEV),
              edge_dst.reshape(GROUP_SIZE, EDGE_DEV),
              edge_mask.reshape(GROUP_SIZE, EDGE_DEV),
              cot_mesh.reshape(GROUP_SIZE, MESH_DEV, LATENT))

    def block_step(carry, blk):
        grad_acc, w1_acc, w2_acc = carry
        mesh_blk, edge_blk, src_blk, dst_blk, mask_blk, cot_blk = blk
        mesh_h = mlp_forward(mesh_blk.astype(jnp.bfloat16), mesh_w1, mesh_w2, mesh_vec)[0].astype(jnp.bfloat16)
        edge_h = mlp_forward(edge_blk.astype(jnp.bfloat16), embed_w1, embed_w2, embed_vec)[0].astype(jnp.bfloat16)
        edge_cat = jnp.concatenate([edge_h, grid_h[src_blk], mesh_h[dst_blk]], axis=1)
        edge_y, edge_saved = mlp_forward(edge_cat, edge_w1, edge_w2, edge_vec)
        keep_col = mask_blk.astype(jnp.float32)[:, None]
        message = keep_col * (edge_h.astype(jnp.float32) + edge_y)
        agg_sum = jax.ops.segment_sum(message, dst_blk, num_segments=MESH_DEV).astype(jnp.bfloat16)
        node_y, node_saved = mlp_forward(jnp.concatenate([mesh_h, agg_sum], axis=1), node_w1, node_w2, node_vec)
        mesh_out_blk = (mesh_h.astype(jnp.float32) + node_y).astype(jnp.bfloat16)
        node_g1 = mlp_backward(cot_blk.astype(jnp.float32), node_w2, node_vec, node_saved)[0]
        agg_grad = jnp.dot(node_g1, node_w1[LATENT:].T, preferred_element_type=jnp.float32)
        edge_g1, edge_g2 = mlp_backward(keep_col * agg_grad[dst_blk], edge_w2, edge_vec, edge_saved)
        w1_acc = w1_acc + jnp.dot(edge_cat.T, edge_g1, preferred_element_type=jnp.float32)
        w2_acc = w2_acc + jnp.dot(edge_saved[1].T, edge_g2, preferred_element_type=jnp.float32)
        src_grad = jnp.dot(edge_g1, edge_w1[LATENT:2 * LATENT].T, preferred_element_type=jnp.float32)
        grad_acc = grad_acc.at[src_blk].add(src_grad)
        return (grad_acc, w1_acc, w2_acc), mesh_out_blk

    init_acc = (jnp.zeros((GRID_ROWS, LATENT), jnp.float32), jnp.zeros((3 * LATENT, LATENT), jnp.float32),
                jnp.zeros((LATENT, LATENT), jnp.float32))
    (edge_part, w1_grad, w2_grad), mesh_out = lax.scan(block_step, init_acc, blocks)
    post_g1 = mlp_backward(cot_grid.astype(jnp.float32), post_w2, post_vec, post_saved)[0]
    grid_cot = cot_grid.astype(jnp.float32) + jnp.dot(post_g1, post_w1.T, preferred_element_type=jnp.float32) + edge_part
    grid_g1 = mlp_backward(grid_cot, grid_w2, grid_vec, grid_saved)[0]
    grid_grad = jnp.dot(grid_g1, grid_w1.T, preferred_element_type=jnp.float32)
    return mesh_out.reshape(MESH_ROWS, LATENT), grid_out, grid_grad, w1_grad, w2_grad
```

```python
import functools

import jax
import jax.numpy as jnp
from jax import lax
from jax.experimental import pallas as pl
from jax.experimental.pallas import tpu as pltpu
from jax.sharding import PartitionSpec as P

NORM_EPS = 1e-5
LANES = 128
SUB = 256
STEP = 1024
BF = jnp.bfloat16
F32 = jnp.float32


def mm(lhs, rhs):
    return jnp.dot(lhs, rhs, preferred_element_type=F32)


def mm_t(lhs, rhs):
    return lax.dot_general(lhs, rhs, (((1,), (1,)), ((), ())), preferred_element_type=F32)


def split3(val):
    hi = val.astype(BF)
    rest = val - hi.astype(F32)
    mid = rest.astype(BF)
    lo = (rest - mid.astype(F32)).astype(BF)
    return hi, mid, lo


def sigmoid(val):
    return 0.5 * jnp.tanh(0.5 * val) + 0.5


def lanes_of(col, width):
    return jnp.concatenate([col] * (width // LANES), axis=1)


def one_hot(ids_row, first, rows):
    row_ids = lax.broadcasted_iota(jnp.int32, (rows, ids_row.shape[1]), 0) + first
    return jnp.where(row_ids == ids_row, 1.0, 0.0).astype(BF)


def norm_fwd(val):
    centred = val - jnp.mean(val, axis=0, keepdims=True)
    inv = lax.rsqrt(jnp.mean(centred * centred, axis=0, keepdims=True) + NORM_EPS)
    return centred * inv, inv


def edge_fwd_kernel(mesh_tiles, table_rows, tile_ref, fit_ref, live_ref, feat_ref, key_ref, em_w1t, em_w2t, em_vec,
                    w1t, w2t, vec, table_t, hm_t, he_out, pre_out, norm_out, inv_out, agg_out):
    step = pl.program_id(0)
    latent = w2t.shape[0]
    shift = 10

    @pl.when(step == 0)
    def _():
        agg_out[...] = jnp.zeros_like(agg_out)

    def body(whole):
        for sub in range(STEP // SUB):
            cols = pl.ds(sub * SUB, SUB)
            vec_at = lambda ref, row: lanes_of(ref[row], SUB)
            key = key_ref[:, cols]
            src = key & (2 ** shift - 1)
            dst = key >> shift
            feat = feat_ref[:, cols].astype(BF)
            pre = mm(em_w1t[...], feat) + vec_at(em_vec, 0)
            act = (pre * sigmoid(pre)).astype(BF)
            normed, _ = norm_fwd(mm(em_w2t[...], act) + vec_at(em_vec, 1))
            he = (normed * vec_at(em_vec, 2) + vec_at(em_vec, 3)).astype(BF)
            he_out[:, cols] = he
            hg = mm(table_t[...], one_hot(src, 0, table_rows)).astype(BF)
            if whole:
                tiles = list(range(mesh_tiles))
                hot = one_hot(dst, 0, mesh_tiles * LANES)
            else:
                first = tile_ref[step * (STEP // SUB) + sub]
                tiles = [first, first + 1]
                hot = one_hot(dst, first * LANES, 2 * LANES)
            window = jnp.concatenate([hm_t[t] for t in tiles], axis=1)
            hm = mm(window, hot).astype(BF)
            pre = mm(w1t[:, :latent], he) + mm(w1t[:, latent:2 * latent], hg) + mm(w1t[:, 2 * latent:], hm)
            pre = pre + vec_at(vec, 0)
            pre_out[:, cols] = pre
            act = (pre * sigmoid(pre)).astype(BF)
            normed, inv = norm_fwd(mm(w2t[...], act) + vec_at(vec, 1))
            norm_out[:, cols] = normed
            inv_out[:, cols] = inv
            msg = he.astype(F32) + (normed * vec_at(vec, 2) + vec_at(vec, 3))
            hi, mid, lo = split3(msg)
            add = mm_t(hi, hot) + mm_t(mid, hot) + mm_t(lo, hot)
            for idx, tile in enumerate(tiles):
                agg_out[tile] += add[:, idx * LANES:(idx + 1) * LANES]

    live = step * STEP < live_ref[0]
    fit = fit_ref[step] == 1

    @pl.when(live & fit)
    def _():
        body(False)

    @pl.when(live & jnp.logical_not(fit))
    def _():
        body(True)


def edge_bwd_kernel(mesh_tiles, table_rows, steps, tile_ref, fit_ref, live_ref, key_ref, he_ref, pre_ref, norm_ref, inv_ref,
                    node_wb, w1b, w2, vec, table_t, both_t, w1_out, w2_out, table_out,
                    g1_buf, g2_buf, act_buf, hm_buf, hot_buf, sum_buf):
    step = pl.program_id(0)
    latent = w2.shape[0]
    shift = 10

    @pl.when(step == 0)
    def _():
        w1_out[...] = jnp.zeros_like(w1_out)
        w2_out[...] = jnp.zeros_like(w2_out)
        sum_buf[...] = jnp.zeros_like(sum_buf)

    def body(whole):
        for sub in range(STEP // SUB):
            cols = pl.ds(sub * SUB, SUB)
            key = key_ref[:, cols]
            src = key & (2 ** shift - 1)
            dst = key >> shift
            if whole:
                tiles = list(range(mesh_tiles))
                hot = one_hot(dst, 0, mesh_tiles * LANES)
            else:
                first = tile_ref[step * (STEP // SUB) + sub]
                tiles = [first, first + 1]
                hot = one_hot(dst, first * LANES, 2 * LANES)
            window = jnp.concatenate([both_t[t] for t in tiles], axis=1)
            both = mm(window, hot).astype(BF)
            hm_buf[:, cols] = both[:latent]
            hot_buf[:, cols] = one_hot(src, 0, table_rows)
            d_norm = mm(node_wb[...], both[latent:]) * lanes_of(vec[2], SUB)
            normed = norm_ref[:, cols]
            d_two = inv_ref[:, cols] * (d_norm - jnp.mean(d_norm, axis=0, keepdims=True)
                                        - normed * jnp.mean(d_norm * normed, axis=0, keepdims=True))
            g_two = d_two.astype(BF)
            g2_buf[:, cols] = g_two
            d_act = mm(w2[...], g_two)
            pre = pre_ref[:, cols]
            sig = sigmoid(pre)
            g1_buf[:, cols] = (d_act * sig * (1.0 + pre * (1.0 - sig))).astype(BF)
            act_buf[:, cols] = (pre * sig).astype(BF)
        w2_out[...] += mm_t(act_buf[...], g2_buf[...])
        g_one = g1_buf[...]
        w1_out[:latent] += mm_t(he_ref[...], g_one)
        w1_out[2 * latent:] += mm_t(hm_buf[...], g_one)
        sum_buf[...] += mm_t(hot_buf[...], g_one)

    live = step * STEP < live_ref[0]
    fit = fit_ref[step] == 1

    @pl.when(live & fit)
    def _():
        body(False)

    @pl.when(live & jnp.logical_not(fit))
    def _():
        body(True)

    @pl.when(step == steps - 1)
    def _():
        hi, mid, lo = split3(sum_buf[...])
        w1_out[latent:2 * latent] = mm(table_t[...], hi) + mm(table_t[...], mid) + mm(table_t[...], lo)
        table_out[...] = mm_t(hi, w1b[...]) + mm_t(mid, w1b[...]) + mm_t(lo, w1b[...])


def mlp_forward(x_in, w_one, w_two, vec_rows):
    pre_one = jnp.dot(x_in, w_one, preferred_element_type=jnp.float32) + vec_rows[0]
    act_bf = jax.nn.silu(pre_one).astype(jnp.bfloat16)
    pre_two = jnp.dot(act_bf, w_two, preferred_element_type=jnp.float32) + vec_rows[1]
    centred = pre_two - jnp.mean(pre_two, axis=-1, keepdims=True)
    inv_std = lax.rsqrt(jnp.mean(centred * centred, axis=-1, keepdims=True) + NORM_EPS)
    normed = centred * inv_std
    return normed * vec_rows[2] + vec_rows[3], (pre_one, act_bf, normed, inv_std)


def mlp_backward(d_out, w_two, vec_rows, saved_acts):
    pre_one, act_bf, normed, inv_std = saved_acts
    d_norm = d_out * vec_rows[2]
    d_two = inv_std * (d_norm - jnp.mean(d_norm, axis=-1, keepdims=True)
                       - normed * jnp.mean(d_norm * normed, axis=-1, keepdims=True))
    g_two = d_two.astype(jnp.bfloat16)
    d_act = jnp.einsum('nj,kj->nk', g_two, w_two, preferred_element_type=jnp.float32)
    sig_pre = jax.nn.sigmoid(pre_one)
    d_one = d_act * sig_pre * (1.0 + pre_one * (1.0 - sig_pre))
    return d_one.astype(jnp.bfloat16), g_two


def whole_spec(arr):
    zeros = (0,) * arr.ndim
    return pl.BlockSpec(arr.shape, lambda i, *_: zeros)


def lane_table(vec_rows):
    return jnp.broadcast_to(vec_rows[:, :, None], vec_rows.shape + (LANES,))


def feature_major(rows):
    return jnp.swapaxes(rows.reshape(-1, LANES, rows.shape[1]), 1, 2)


def solution(mesh):
    groups = mesh.shape['graph']
    row_spec = P(('batch', 'graph'), None)
    flat_spec = P(('batch', 'graph'))
    rep_spec = P(None, None)
    down_perm = [(src_dev, src_dev - 1) for src_dev in range(1, groups)]
    up_perm = [(src_dev, src_dev + 1) for src_dev in range(groups - 1)]

    def device_step(grid_in, mesh_in, edge_in, edge_src, edge_dst, edge_mask, grid_w1, grid_w2, grid_vec,
                    mesh_w1, mesh_w2, mesh_vec, embed_w1, embed_w2, embed_vec, edge_w1, edge_w2, edge_vec,
                    node_w1, node_w2, node_vec, post_w1, post_w2, post_vec, cot_mesh, cot_grid):
        band_rows = grid_in.shape[0]
        halo_rows = band_rows // 4
        latent = grid_w2.shape[1]
        mesh_rows = mesh_in.shape[0]
        edges = edge_in.shape[0]
        table_rows = band_rows + 2 * halo_rows
        mesh_tiles = mesh_rows // LANES
        steps = edges // STEP
        band_index = lax.axis_index('graph')

        grid_y, grid_saved = mlp_forward(grid_in.astype(BF), grid_w1, grid_w2, grid_vec)
        grid_h = grid_y.astype(BF)
        from_above = lax.ppermute(grid_h[:halo_rows], 'graph', down_perm)
        from_below = lax.ppermute(grid_h[band_rows - halo_rows:], 'graph', up_perm)

        local_src = edge_src - (band_index * band_rows - halo_rows)
        real = edge_mask != 0
        key = jnp.where(real, edge_dst * 1024 + local_src, mesh_rows * 1024)
        feat_t = edge_in.T
        key, f0, f1, f2, f3 = lax.sort((key, feat_t[0], feat_t[1], feat_t[2], feat_t[3]), num_keys=1, is_stable=False)
        zero_row = jnp.zeros_like(f0)
        feats = jnp.stack([f0, f1, f2, f3, zero_row, zero_row, zero_row, zero_row])
        live = jnp.sum(real.astype(jnp.int32)).reshape(1)
        dst_sorted = (key >> 10).reshape(-1, SUB)
        low = jnp.min(dst_sorted, axis=1)
        high = jnp.max(jnp.where(dst_sorted < mesh_rows, dst_sorted, 0), axis=1)
        first_tile = jnp.minimum(low // LANES, mesh_tiles - 2)
        fits = ((high - first_tile * LANES) < 2 * LANES).reshape(steps, STEP // SUB)
        fits = jnp.all(fits, axis=1).astype(jnp.int32)
        key_row = key.reshape(1, edges)

        mesh_h = mlp_forward(mesh_in.astype(BF), mesh_w1, mesh_w2, mesh_vec)[0].astype(BF)
        table_t = jnp.concatenate([from_below, grid_h, from_above], axis=0).T
        hm_t = feature_major(mesh_h)
        em_w1t = jnp.pad(embed_w1, ((0, 8 - embed_w1.shape[0]), (0, 0))).T
        edge_vec_t = lane_table(edge_vec)

        lane_block = lambda rows: pl.BlockSpec((rows, STEP), lambda i, *_: (0, i))
        fwd_in = (feats, key_row, em_w1t, embed_w2.T, lane_table(embed_vec), edge_w1.T, edge_w2.T, edge_vec_t, table_t, hm_t)
        he_t, pre_t, norm_t, inv_t, agg_t = pl.pallas_call(
            functools.partial(edge_fwd_kernel, mesh_tiles, table_rows),
            grid_spec=pltpu.PrefetchScalarGridSpec(
                num_scalar_prefetch=3, grid=(steps,),
                in_specs=[lane_block(8), lane_block(1)] + [whole_spec(a) for a in fwd_in[2:]],
                out_specs=[lane_block(latent), lane_block(latent), lane_block(latent), lane_block(1),
                           pl.BlockSpec((mesh_tiles, latent, LANES), lambda i, *_: (0, 0, 0))]),
            out_shape=[jax.ShapeDtypeStruct((latent, edges), BF), jax.ShapeDtypeStruct((latent, edges), F32),
                       jax.ShapeDtypeStruct((latent, edges), F32), jax.ShapeDtypeStruct((1, edges), F32),
                       jax.ShapeDtypeStruct((mesh_tiles, latent, LANES), F32)],
            compiler_params=pltpu.CompilerParams(dimension_semantics=("arbitrary",), vmem_limit_bytes=60 * 2 ** 20),
            cost_estimate=pl.CostEstimate(flops=9 * 2 * edges * latent * latent, bytes_accessed=64 * 2 ** 20,
                                          transcendentals=2 * edges * latent),
            name="edge_fwd",
        )(first_tile, fits, live, *fwd_in)

        agg_sum = jnp.swapaxes(agg_t, 1, 2).reshape(mesh_rows, latent).astype(BF)
        node_y, node_saved = mlp_forward(jnp.concatenate([mesh_h, agg_sum], axis=1), node_w1, node_w2, node_vec)
        mesh_out = (mesh_h.astype(F32) + node_y).astype(BF)
        node_g1 = mlp_backward(cot_mesh.astype(F32), node_w2, node_vec, node_saved)[0]

        both_t = jnp.concatenate([hm_t, feature_major(node_g1)], axis=1)
        w1b = edge_w1[latent:2 * latent]
        bwd_in = (key_row, he_t, pre_t, norm_t, inv_t, node_w1[latent:], w1b, edge_w2, edge_vec_t, table_t, both_t)
        w1_part, w2_part, table_grad = pl.pallas_call(
            functools.partial(edge_bwd_kernel, mesh_tiles, table_rows, steps),
            grid_spec=pltpu.PrefetchScalarGridSpec(
                num_scalar_prefetch=3, grid=(steps,),
                in_specs=[lane_block(1), lane_block(latent), lane_block(latent), lane_block(latent), lane_block(1)]
                + [whole_spec(a) for a in bwd_in[5:]],
                out_specs=[pl.BlockSpec((3 * latent, latent), lambda i, *_: (0, 0)),
                           pl.BlockSpec((latent, latent), lambda i, *_: (0, 0)),
                           pl.BlockSpec((table_rows, latent), lambda i, *_: (0, 0))],
                scratch_shapes=[pltpu.VMEM((latent, STEP), BF)] * 4
                + [pltpu.VMEM((table_rows, STEP), BF), pltpu.VMEM((table_rows, latent), F32)]),
            out_shape=[jax.ShapeDtypeStruct((3 * latent, latent), F32), jax.ShapeDtypeStruct((latent, latent), F32),
                       jax.ShapeDtypeStruct((table_rows, latent), F32)],
            compiler_params=pltpu.CompilerParams(dimension_semantics=("arbitrary",), vmem_limit_bytes=60 * 2 ** 20),
            cost_estimate=pl.CostEstimate(flops=15 * edges * latent * latent, bytes_accessed=64 * 2 ** 20,
                                          transcendentals=edges * latent),
            name="edge_bwd",
        )(first_tile, fits, live, *bwd_in)

        w_parts = jnp.concatenate([w1_part.reshape(groups, -1, latent), w2_part.reshape(groups, -1, latent)], axis=1)
        w_sum = lax.psum_scatter(w_parts, 'graph', scatter_dimension=0, tiled=True)[0]
        w1_grad, w2_grad = w_sum[:w1_part.shape[0] // groups], w_sum[w1_part.shape[0] // groups:]

        tail_grad = lax.ppermute(table_grad[:halo_rows], 'graph', down_perm)
        head_grad = lax.ppermute(table_grad[band_rows + halo_rows:], 'graph', up_perm)
        post_y, post_saved = mlp_forward(grid_h, post_w1, post_w2, post_vec)
        grid_out = (grid_h.astype(F32) + post_y).astype(BF)
        post_g1 = mlp_backward(cot_grid.astype(F32), post_w2, post_vec, post_saved)[0]
        grid_cot = cot_grid.astype(F32) + jnp.einsum('nj,kj->nk', post_g1, post_w1, preferred_element_type=F32)
        edge_part = table_grad[halo_rows:band_rows + halo_rows] + jnp.concatenate(
            [head_grad, jnp.zeros((band_rows - 2 * halo_rows, latent), F32), tail_grad], axis=0)
        grid_g1 = mlp_backward(grid_cot + edge_part, grid_w2, grid_vec, grid_saved)[0]
        grid_grad = jnp.einsum('nj,kj->nk', grid_g1, grid_w1, preferred_element_type=F32)
        return mesh_out, grid_out, grid_grad, w1_grad, w2_grad

    in_specs = (row_spec, row_spec, row_spec, flat_spec, flat_spec, flat_spec) + (rep_spec,) * 18 + (row_spec, row_spec)
    return jax.shard_map(device_step, mesh=mesh, in_specs=in_specs, out_specs=(row_spec,) * 5, check_vma=False)
```

```python
import functools

import jax
import jax.numpy as jnp
from jax import lax
from jax.experimental import pallas as pl
from jax.experimental.pallas import tpu as pltpu
from jax.sharding import PartitionSpec as P

NORM_EPS = 1e-5
LANES = 128
SUB = 256
STEP = 1024
BF = jnp.bfloat16
F32 = jnp.float32
MESH = pl.DeviceIdType.MESH


def mm(lhs, rhs):
    return jnp.dot(lhs, rhs, preferred_element_type=F32)


def mm_t(lhs, rhs):
    return lax.dot_general(lhs, rhs, (((1,), (1,)), ((), ())), preferred_element_type=F32)


def split3(val):
    hi = val.astype(BF)
    rest = val - hi.astype(F32)
    mid = rest.astype(BF)
    lo = (rest - mid.astype(F32)).astype(BF)
    return hi, mid, lo


def sigmoid(val):
    return 0.5 * jnp.tanh(0.5 * val) + 0.5


def lanes_of(col, width):
    return jnp.concatenate([col] * (width // LANES), axis=1)


def one_hot(ids_row, first, rows):
    row_ids = lax.broadcasted_iota(jnp.int32, (rows, ids_row.shape[1]), 0) + first
    return jnp.where(row_ids == ids_row, 1.0, 0.0).astype(BF)


def norm_fwd(val):
    centred = val - jnp.mean(val, axis=0, keepdims=True)
    inv = lax.rsqrt(jnp.mean(centred * centred, axis=0, keepdims=True) + NORM_EPS)
    return centred * inv, inv


def edge_fwd_kernel(mesh_tiles, table_rows, tile_ref, fit_ref, live_ref, feat_ref, key_ref, em_w1t, em_w2t, em_vec,
                    w1t, w2t, vec, table_t, hm_t, he_out, pre_out, norm_out, inv_out, agg_out):
    step = pl.program_id(0)
    latent = w2t.shape[0]
    shift = 10

    @pl.when(step == 0)
    def _():
        agg_out[...] = jnp.zeros_like(agg_out)

    def body(whole):
        for sub in range(STEP // SUB):
            cols = pl.ds(sub * SUB, SUB)
            vec_at = lambda ref, row: lanes_of(ref[row], SUB)
            key = key_ref[:, cols]
            src = key & (2 ** shift - 1)
            dst = key >> shift
            feat = feat_ref[:, cols].astype(BF)
            pre = mm(em_w1t[...], feat) + vec_at(em_vec, 0)
            act = (pre * sigmoid(pre)).astype(BF)
            normed, _ = norm_fwd(mm(em_w2t[...], act) + vec_at(em_vec, 1))
            he = (normed * vec_at(em_vec, 2) + vec_at(em_vec, 3)).astype(BF)
            he_out[:, cols] = he
            hg = mm(table_t[...], one_hot(src, 0, table_rows)).astype(BF)
            if whole:
                tiles = list(range(mesh_tiles))
                hot = one_hot(dst, 0, mesh_tiles * LANES)
            else:
                first = tile_ref[step * (STEP // SUB) + sub]
                tiles = [first, first + 1]
                hot = one_hot(dst, first * LANES, 2 * LANES)
            window = jnp.concatenate([hm_t[t] for t in tiles], axis=1)
            hm = mm(window, hot).astype(BF)
            pre = mm(w1t[:, :latent], he) + mm(w1t[:, latent:2 * latent], hg) + mm(w1t[:, 2 * latent:], hm)
            pre = pre + vec_at(vec, 0)
            pre_out[:, cols] = pre
            act = (pre * sigmoid(pre)).astype(BF)
            normed, inv = norm_fwd(mm(w2t[...], act) + vec_at(vec, 1))
            norm_out[:, cols] = normed
            inv_out[:, cols] = inv
            msg = he.astype(F32) + (normed * vec_at(vec, 2) + vec_at(vec, 3))
            hi, mid, lo = split3(msg)
            add = mm_t(hi, hot) + mm_t(mid, hot) + mm_t(lo, hot)
            for idx, tile in enumerate(tiles):
                agg_out[tile] += add[:, idx * LANES:(idx + 1) * LANES]

    live = step * STEP < live_ref[0]
    fit = fit_ref[step] == 1

    @pl.when(live & fit)
    def _():
        body(False)

    @pl.when(live & jnp.logical_not(fit))
    def _():
        body(True)


def edge_bwd_kernel(mesh_tiles, table_rows, steps, tile_ref, fit_ref, live_ref, key_ref, he_ref, pre_ref, norm_ref, inv_ref,
                    node_wb, w1b, w2, vec, table_t, both_t, w1_out, w2_out, table_out,
                    g1_buf, g2_buf, act_buf, hm_buf, hot_buf, sum_buf):
    step = pl.program_id(0)
    latent = w2.shape[0]
    shift = 10

    @pl.when(step == 0)
    def _():
        w1_out[...] = jnp.zeros_like(w1_out)
        w2_out[...] = jnp.zeros_like(w2_out)
        sum_buf[...] = jnp.zeros_like(sum_buf)

    def body(whole):
        for sub in range(STEP // SUB):
            cols = pl.ds(sub * SUB, SUB)
            key = key_ref[:, cols]
            src = key & (2 ** shift - 1)
            dst = key >> shift
            if whole:
                tiles = list(range(mesh_tiles))
                hot = one_hot(dst, 0, mesh_tiles * LANES)
            else:
                first = tile_ref[step * (STEP // SUB) + sub]
                tiles = [first, first + 1]
                hot = one_hot(dst, first * LANES, 2 * LANES)
            window = jnp.concatenate([both_t[t] for t in tiles], axis=1)
            both = mm(window, hot).astype(BF)
            hm_buf[:, cols] = both[:latent]
            hot_buf[:, cols] = one_hot(src, 0, table_rows)
            d_norm = mm(node_wb[...], both[latent:]) * lanes_of(vec[2], SUB)
            normed = norm_ref[:, cols]
            d_two = inv_ref[:, cols] * (d_norm - jnp.mean(d_norm, axis=0, keepdims=True)
                                        - normed * jnp.mean(d_norm * normed, axis=0, keepdims=True))
            g_two = d_two.astype(BF)
            g2_buf[:, cols] = g_two
            d_act = mm(w2[...], g_two)
            pre = pre_ref[:, cols]
            sig = sigmoid(pre)
            g1_buf[:, cols] = (d_act * sig * (1.0 + pre * (1.0 - sig))).astype(BF)
            act_buf[:, cols] = (pre * sig).astype(BF)
        w2_out[...] += mm_t(act_buf[...], g2_buf[...])
        g_one = g1_buf[...]
        w1_out[:latent] += mm_t(he_ref[...], g_one)
        w1_out[2 * latent:] += mm_t(hm_buf[...], g_one)
        sum_buf[...] += mm_t(hot_buf[...], g_one)

    live = step * STEP < live_ref[0]
    fit = fit_ref[step] == 1

    @pl.when(live & fit)
    def _():
        body(False)

    @pl.when(live & jnp.logical_not(fit))
    def _():
        body(True)

    @pl.when(step == steps - 1)
    def _():
        hi, mid, lo = split3(sum_buf[...])
        w1_out[latent:2 * latent] = mm(table_t[...], hi) + mm(table_t[...], mid) + mm(table_t[...], lo)
        table_out[...] = mm_t(hi, w1b[...]) + mm_t(mid, w1b[...]) + mm_t(lo, w1b[...])


STRIDE = {'z': 32, 'y': 8, 'x': 2}
ORDERS = (('x', 'y', 'z'), ('y', 'z', 'x'), ('z', 'x', 'y'))
DIM = 4


def scatter_kernel(w1_ref, w2_ref, g1_out, g2_out, pair1, pair2, *scratch):
    full = scratch[0:3]
    recv = (scratch[3:6], scratch[6:9], scratch[9:12])
    part = (scratch[12:15], scratch[15:18])
    done1, done2, pair_send, pair_recv, hop_send, hop_recv = scratch[18:]
    me = lax.axis_index('graph')
    core = me % 2
    coord = {name: (me // stride) % DIM for name, stride in STRIDE.items()}
    partner = me + 1 - 2 * core

    def peer(name, hop):
        there = (coord[name] + hop) % DIM
        return there, me + (there - coord[name]) * STRIDE[name]

    barrier = pltpu.get_barrier_semaphore()
    others = [partner] + [peer(name, hop)[1] for name in STRIDE for hop in range(1, DIM)]
    for other in others:
        pl.semaphore_signal(barrier, inc=1, device_id={'graph': other}, device_id_type=MESH)
    pl.semaphore_wait(barrier, len(others))

    half = w1_ref.shape[-1] // 2
    mine = pl.multiple_of(core * half, half)
    theirs = pl.multiple_of((1 - core) * half, half)

    def to_partner(src, dst, slot):
        copy = pltpu.make_async_remote_copy(src_ref=src, dst_ref=dst, send_sem=pair_send.at[slot], recv_sem=pair_recv.at[slot],
                                            device_id={'graph': partner}, device_id_type=MESH)
        copy.start()
        return copy

    first = [to_partner(w1_ref.at[:, :, :, :, pl.ds(theirs, half)], pair1, 0),
             to_partner(w2_ref.at[:, :, :, :, pl.ds(theirs, half)], pair2, 1)]
    first[0].wait()
    quarter = half // 2
    full[0][...] = w1_ref[:, :, :, :, pl.ds(mine, quarter)] + pair1[:, :, :, :, :quarter]
    full[1][...] = w1_ref[:, :, :, :, pl.ds(mine + quarter, quarter)] + pair1[:, :, :, :, quarter:]
    first[1].wait()
    full[2][...] = w2_ref[:, :, :, :, pl.ds(mine, half)] + pair2[...]

    left = [list(STRIDE) for _ in range(3)]
    held = list(full)

    def at(color, name, index):
        pos = left[color].index(name)
        return (slice(None),) * pos + (index,)

    for stage in range(3):
        copies = []
        for color in range(3):
            name = ORDERS[color][stage]
            for hop in range(1, DIM):
                there, device = peer(name, hop)
                copy = pltpu.make_async_remote_copy(
                    src_ref=held[color].at[at(color, name, there)], dst_ref=recv[stage][color].at[hop - 1],
                    send_sem=hop_send.at[stage, color, hop - 1], recv_sem=hop_recv.at[stage, color, hop - 1],
                    device_id={'graph': device}, device_id_type=MESH)
                copy.start()
                copies.append(copy)
        for color in range(3):
            for copy in copies[3 * color:3 * color + 3]:
                copy.wait()
            name = ORDERS[color][stage]
            got = recv[stage][color]
            total = held[color][at(color, name, coord[name])] + got[0] + got[1] + got[2]
            left[color].remove(name)
            if stage < 2:
                part[stage][color][...] = total
                held[color] = part[stage][color]
            elif color == 2:
                done2[core] = total
            else:
                done1[core, :, color * quarter:(color + 1) * quarter] = total

    last = [to_partner(done1.at[core], done1.at[core], 2), to_partner(done2.at[core], done2.at[core], 3)]
    for copy in last:
        copy.wait()
    for done, out in ((done1, g1_out), (done2, g2_out)):
        rows = out.shape[0]
        whole = jnp.concatenate([done[0], done[1]], axis=1)
        out[...] = jnp.where(core == 0, whole[:rows], whole[rows:])


def scatter_call(w1, w2):
    rows1, rows2, cols = w1.shape[-2], w2.shape[-2], w1.shape[-1]
    half, quarter = cols // 2, cols // 4
    tail = ((rows1, quarter), (rows1, quarter), (rows2, half))
    scratch = [pltpu.VMEM((DIM,) * 3 + (rows1, half), F32), pltpu.VMEM((DIM,) * 3 + (rows2, half), F32)]
    scratch += [pltpu.VMEM((DIM,) * 3 + t, F32) for t in tail]
    for stage in range(3):
        scratch += [pltpu.VMEM((3,) + (DIM,) * (2 - stage) + t, F32) for t in tail]
    for stage in range(2):
        scratch += [pltpu.VMEM((DIM,) * (2 - stage) + t, F32) for t in tail]
    scratch += [pltpu.VMEM((2, rows1, half), F32), pltpu.VMEM((2, rows2, half), F32),
                pltpu.SemaphoreType.DMA((4,)), pltpu.SemaphoreType.DMA((4,)),
                pltpu.SemaphoreType.DMA((3, 3, 3)), pltpu.SemaphoreType.DMA((3, 3, 3))]
    vm = pl.BlockSpec(memory_space=pltpu.VMEM)
    return pl.pallas_call(
        scatter_kernel,
        in_specs=[vm, vm], out_specs=[vm, vm],
        out_shape=[jax.ShapeDtypeStruct((rows1 // 2, cols), F32), jax.ShapeDtypeStruct((rows2 // 2, cols), F32)],
        scratch_shapes=scratch,
        compiler_params=pltpu.CompilerParams(collective_id=0, has_side_effects=True, vmem_limit_bytes=40 * 2 ** 20),
        name="weight_scatter",
    )(w1, w2)


def mlp_forward(x_in, w_one, w_two, vec_rows):
    pre_one = jnp.dot(x_in, w_one, preferred_element_type=jnp.float32) + vec_rows[0]
    act_bf = jax.nn.silu(pre_one).astype(jnp.bfloat16)
    pre_two = jnp.dot(act_bf, w_two, preferred_element_type=jnp.float32) + vec_rows[1]
    centred = pre_two - jnp.mean(pre_two, axis=-1, keepdims=True)
    inv_std = lax.rsqrt(jnp.mean(centred * centred, axis=-1, keepdims=True) + NORM_EPS)
    normed = centred * inv_std
    return normed * vec_rows[2] + vec_rows[3], (pre_one, act_bf, normed, inv_std)


def mlp_backward(d_out, w_two, vec_rows, saved_acts):
    pre_one, act_bf, normed, inv_std = saved_acts
    d_norm = d_out * vec_rows[2]
    d_two = inv_std * (d_norm - jnp.mean(d_norm, axis=-1, keepdims=True)
                       - normed * jnp.mean(d_norm * normed, axis=-1, keepdims=True))
    g_two = d_two.astype(jnp.bfloat16)
    d_act = jnp.einsum('nj,kj->nk', g_two, w_two, preferred_element_type=jnp.float32)
    sig_pre = jax.nn.sigmoid(pre_one)
    d_one = d_act * sig_pre * (1.0 + pre_one * (1.0 - sig_pre))
    return d_one.astype(jnp.bfloat16), g_two


def whole_spec(arr):
    zeros = (0,) * arr.ndim
    return pl.BlockSpec(arr.shape, lambda i, *_: zeros)


def lane_table(vec_rows):
    return jnp.broadcast_to(vec_rows[:, :, None], vec_rows.shape + (LANES,))


def feature_major(rows):
    return jnp.swapaxes(rows.reshape(-1, LANES, rows.shape[1]), 1, 2)


def solution(mesh):
    groups = mesh.shape['graph']
    row_spec = P(('batch', 'graph'), None)
    flat_spec = P(('batch', 'graph'))
    rep_spec = P(None, None)
    down_perm = [(src_dev, src_dev - 1) for src_dev in range(1, groups)]
    up_perm = [(src_dev, src_dev + 1) for src_dev in range(groups - 1)]

    def device_step(grid_in, mesh_in, edge_in, edge_src, edge_dst, edge_mask, grid_w1, grid_w2, grid_vec,
                    mesh_w1, mesh_w2, mesh_vec, embed_w1, embed_w2, embed_vec, edge_w1, edge_w2, edge_vec,
                    node_w1, node_w2, node_vec, post_w1, post_w2, post_vec, cot_mesh, cot_grid):
        band_rows = grid_in.shape[0]
        halo_rows = band_rows // 4
        latent = grid_w2.shape[1]
        mesh_rows = mesh_in.shape[0]
        edges = edge_in.shape[0]
        table_rows = band_rows + 2 * halo_rows
        mesh_tiles = mesh_rows // LANES
        steps = edges // STEP
        band_index = lax.axis_index('graph')

        grid_y, grid_saved = mlp_forward(grid_in.astype(BF), grid_w1, grid_w2, grid_vec)
        grid_h = grid_y.astype(BF)
        from_above = lax.ppermute(grid_h[:halo_rows], 'graph', down_perm)
        from_below = lax.ppermute(grid_h[band_rows - halo_rows:], 'graph', up_perm)

        local_src = edge_src - (band_index * band_rows - halo_rows)
        real = edge_mask != 0
        key = jnp.where(real, edge_dst * 1024 + local_src, mesh_rows * 1024)
        feat_t = edge_in.T
        key, f0, f1, f2, f3 = lax.sort((key, feat_t[0], feat_t[1], feat_t[2], feat_t[3]), num_keys=1, is_stable=False)
        zero_row = jnp.zeros_like(f0)
        feats = jnp.stack([f0, f1, f2, f3, zero_row, zero_row, zero_row, zero_row])
        live = jnp.sum(real.astype(jnp.int32)).reshape(1)
        dst_sorted = (key >> 10).reshape(-1, SUB)
        low = jnp.min(dst_sorted, axis=1)
        high = jnp.max(jnp.where(dst_sorted < mesh_rows, dst_sorted, 0), axis=1)
        first_tile = jnp.minimum(low // LANES, mesh_tiles - 2)
        fits = ((high - first_tile * LANES) < 2 * LANES).reshape(steps, STEP // SUB)
        fits = jnp.all(fits, axis=1).astype(jnp.int32)
        key_row = key.reshape(1, edges)

        mesh_h = mlp_forward(mesh_in.astype(BF), mesh_w1, mesh_w2, mesh_vec)[0].astype(BF)
        table_t = jnp.concatenate([from_below, grid_h, from_above], axis=0).T
        hm_t = feature_major(mesh_h)
        em_w1t = jnp.pad(embed_w1, ((0, 8 - embed_w1.shape[0]), (0, 0))).T
        edge_vec_t = lane_table(edge_vec)

        lane_block = lambda rows: pl.BlockSpec((rows, STEP), lambda i, *_: (0, i))
        fwd_in = (feats, key_row, em_w1t, embed_w2.T, lane_table(embed_vec), edge_w1.T, edge_w2.T, edge_vec_t, table_t, hm_t)
        he_t, pre_t, norm_t, inv_t, agg_t = pl.pallas_call(
            functools.partial(edge_fwd_kernel, mesh_tiles, table_rows),
            grid_spec=pltpu.PrefetchScalarGridSpec(
                num_scalar_prefetch=3, grid=(steps,),
                in_specs=[lane_block(8), lane_block(1)] + [whole_spec(a) for a in fwd_in[2:]],
                out_specs=[lane_block(latent), lane_block(latent), lane_block(latent), lane_block(1),
                           pl.BlockSpec((mesh_tiles, latent, LANES), lambda i, *_: (0, 0, 0))]),
            out_shape=[jax.ShapeDtypeStruct((latent, edges), BF), jax.ShapeDtypeStruct((latent, edges), F32),
                       jax.ShapeDtypeStruct((latent, edges), F32), jax.ShapeDtypeStruct((1, edges), F32),
                       jax.ShapeDtypeStruct((mesh_tiles, latent, LANES), F32)],
            compiler_params=pltpu.CompilerParams(dimension_semantics=("arbitrary",), vmem_limit_bytes=60 * 2 ** 20),
            cost_estimate=pl.CostEstimate(flops=9 * 2 * edges * latent * latent, bytes_accessed=64 * 2 ** 20,
                                          transcendentals=2 * edges * latent),
            name="edge_fwd",
        )(first_tile, fits, live, *fwd_in)

        agg_sum = jnp.swapaxes(agg_t, 1, 2).reshape(mesh_rows, latent).astype(BF)
        node_y, node_saved = mlp_forward(jnp.concatenate([mesh_h, agg_sum], axis=1), node_w1, node_w2, node_vec)
        mesh_out = (mesh_h.astype(F32) + node_y).astype(BF)
        node_g1 = mlp_backward(cot_mesh.astype(F32), node_w2, node_vec, node_saved)[0]

        both_t = jnp.concatenate([hm_t, feature_major(node_g1)], axis=1)
        w1b = edge_w1[latent:2 * latent]
        bwd_in = (key_row, he_t, pre_t, norm_t, inv_t, node_w1[latent:], w1b, edge_w2, edge_vec_t, table_t, both_t)
        w1_part, w2_part, table_grad = pl.pallas_call(
            functools.partial(edge_bwd_kernel, mesh_tiles, table_rows, steps),
            grid_spec=pltpu.PrefetchScalarGridSpec(
                num_scalar_prefetch=3, grid=(steps,),
                in_specs=[lane_block(1), lane_block(latent), lane_block(latent), lane_block(latent), lane_block(1)]
                + [whole_spec(a) for a in bwd_in[5:]],
                out_specs=[pl.BlockSpec((3 * latent, latent), lambda i, *_: (0, 0)),
                           pl.BlockSpec((latent, latent), lambda i, *_: (0, 0)),
                           pl.BlockSpec((table_rows, latent), lambda i, *_: (0, 0))],
                scratch_shapes=[pltpu.VMEM((latent, STEP), BF)] * 4
                + [pltpu.VMEM((table_rows, STEP), BF), pltpu.VMEM((table_rows, latent), F32)]),
            out_shape=[jax.ShapeDtypeStruct((3 * latent, latent), F32), jax.ShapeDtypeStruct((latent, latent), F32),
                       jax.ShapeDtypeStruct((table_rows, latent), F32)],
            compiler_params=pltpu.CompilerParams(dimension_semantics=("arbitrary",), vmem_limit_bytes=60 * 2 ** 20),
            cost_estimate=pl.CostEstimate(flops=15 * edges * latent * latent, bytes_accessed=64 * 2 ** 20,
                                          transcendentals=edges * latent),
            name="edge_bwd",
        )(first_tile, fits, live, *bwd_in)

        chips = (DIM, DIM, DIM)
        w1_grad, w2_grad = scatter_call(w1_part.reshape(chips + (-1, latent)), w2_part.reshape(chips + (-1, latent)))

        tail_grad = lax.ppermute(table_grad[:halo_rows], 'graph', down_perm)
        head_grad = lax.ppermute(table_grad[band_rows + halo_rows:], 'graph', up_perm)
        post_y, post_saved = mlp_forward(grid_h, post_w1, post_w2, post_vec)
        grid_out = (grid_h.astype(F32) + post_y).astype(BF)
        post_g1 = mlp_backward(cot_grid.astype(F32), post_w2, post_vec, post_saved)[0]
        grid_cot = cot_grid.astype(F32) + jnp.einsum('nj,kj->nk', post_g1, post_w1, preferred_element_type=F32)
        edge_part = table_grad[halo_rows:band_rows + halo_rows] + jnp.concatenate(
            [head_grad, jnp.zeros((band_rows - 2 * halo_rows, latent), F32), tail_grad], axis=0)
        grid_g1 = mlp_backward(grid_cot + edge_part, grid_w2, grid_vec, grid_saved)[0]
        grid_grad = jnp.einsum('nj,kj->nk', grid_g1, grid_w1, preferred_element_type=F32)
        return mesh_out, grid_out, grid_grad, w1_grad, w2_grad

    in_specs = (row_spec, row_spec, row_spec, flat_spec, flat_spec, flat_spec) + (rep_spec,) * 18 + (row_spec, row_spec)
    return jax.shard_map(device_step, mesh=mesh, in_specs=in_specs, out_specs=(row_spec,) * 5, check_vma=False)
```

```python
import jax
import jax.numpy as jnp
from jax import lax
from jax.experimental import pallas as pl
from jax.experimental.pallas import tpu as pltpu
from jax.sharding import PartitionSpec as P

NORM_EPS = 1e-5
LANES = 128
SUB = 512
STEP = 1024
KEY_BITS = 10
BF = jnp.bfloat16
F32 = jnp.float32
MESH = pl.DeviceIdType.MESH


def mm(lhs, rhs):
    return jnp.dot(lhs, rhs, preferred_element_type=F32)


def mm_t(lhs, rhs):
    return lax.dot_general(lhs, rhs, (((1,), (1,)), ((), ())), preferred_element_type=F32)


def split3(val):
    hi = val.astype(BF)
    rest = val - hi.astype(F32)
    mid = rest.astype(BF)
    lo = (rest - mid.astype(F32)).astype(BF)
    return hi, mid, lo


def sigmoid(val):
    return 0.5 * jnp.tanh(0.5 * val) + 0.5


def lanes_of(col, width):
    return jnp.concatenate([col] * (width // LANES), axis=1)


def one_hot(ids_row, first, rows):
    row_ids = lax.broadcasted_iota(jnp.int32, (rows, ids_row.shape[1]), 0) + first
    return jnp.where(row_ids == ids_row, 1.0, 0.0).astype(BF)


def norm_fwd(val):
    mean = jnp.mean(val, axis=0, keepdims=True)
    centred = val - mean
    inv = lax.rsqrt(jnp.mean(centred * centred, axis=0, keepdims=True) + NORM_EPS)
    return centred * inv, mean, inv


def norm_bwd(d_norm, normed, inv):
    return inv * (d_norm - jnp.mean(d_norm, axis=0, keepdims=True)
                  - normed * jnp.mean(d_norm * normed, axis=0, keepdims=True))


def edge_kernel(first_ref, fit_ref, live_ref, feat_ref, key_ref, mesh_x, below, band, above, small_w, em_w2, mesh_w2,
                w1, w2, node_w1, node_w2, vecs, cot_ref, mesh_out, w1_out, w2_out, table_out,
                em_w2t, w1t, w2t, table_t, both_t, vec_b, pre_buf, he_buf, mean_buf, inv_buf, agg_buf,
                g1_buf, g2_buf, act_buf, hm_buf, hot_buf):
    latent = w2.shape[0]
    table_rows = table_t.shape[1]
    mesh_tiles = both_t.shape[0]
    per_sub = SUB // LANES
    eye = one_hot(lax.broadcasted_iota(jnp.int32, (1, latent), 1), 0, latent)
    turned = lambda val: mm_t(eye, val).astype(BF)

    em_w2t[...] = turned(em_w2[...])
    w2t[...] = turned(w2[...])
    for part in range(3):
        w1t[:, part * latent:(part + 1) * latent] = turned(w1[part * latent:(part + 1) * latent])
    at = 0
    for piece in (below, band, above):
        rows = piece.shape[0]
        table_t[:, at:at + rows] = turned(piece[...])
        at += rows
    cols = jnp.transpose(vecs[...])
    col = lambda mlp, row: cols[:, 4 * mlp + row:4 * mlp + row + 1]
    for row in range(4):
        vec_b[row] = jnp.broadcast_to(col(0, row), (latent, LANES))
        vec_b[4 + row] = jnp.broadcast_to(col(2, row), (latent, LANES))
    small_t = turned(small_w[...])
    agg_buf[...] = jnp.zeros_like(agg_buf)
    w1_out[...] = jnp.zeros_like(w1_out)
    w2_out[...] = jnp.zeros_like(w2_out)
    table_out[...] = jnp.zeros_like(table_out)

    mesh_w2t = turned(mesh_w2[...])
    for blk in range(mesh_tiles // per_sub):
        pre = mm(small_t[:, 8:], mesh_x[:, blk * SUB:(blk + 1) * SUB].astype(BF)) + col(1, 0)
        act = (pre * sigmoid(pre)).astype(BF)
        normed, _, _ = norm_fwd(mm(mesh_w2t, act) + col(1, 1))
        hm = (normed * col(1, 2) + col(1, 3)).astype(BF)
        for idx in range(per_sub):
            both_t[blk * per_sub + idx, :latent] = hm[:, idx * LANES:(idx + 1) * LANES]

    vec_at = lambda row: lanes_of(vec_b[row], SUB)

    def edges_of(sub, whole):
        span = pl.ds(pl.multiple_of(sub * SUB, SUB), SUB)
        key = key_ref[:, span]
        dst = key >> KEY_BITS
        if whole:
            tiles = list(range(mesh_tiles))
            hot = one_hot(dst, 0, mesh_tiles * LANES)
        else:
            first = first_ref[sub]
            tiles = [first, first + 1]
            hot = one_hot(dst, first * LANES, 2 * LANES)
        return span, one_hot(key & (2 ** KEY_BITS - 1), 0, table_rows), tiles, hot

    def forward(sub, whole):
        span, src_hot, tiles, hot = edges_of(sub, whole)
        pre = mm(small_t[:, :8], feat_ref[:, span].astype(BF)) + vec_at(0)
        act = (pre * sigmoid(pre)).astype(BF)
        normed, _, _ = norm_fwd(mm(em_w2t[...], act) + vec_at(1))
        he = (normed * vec_at(2) + vec_at(3)).astype(BF)
        he_buf[:, span] = he
        hg = mm(table_t[...], src_hot).astype(BF)
        hm = mm(jnp.concatenate([both_t[t, :latent] for t in tiles], axis=1), hot).astype(BF)
        pre = mm(w1t[:, :latent], he) + mm(w1t[:, latent:2 * latent], hg) + mm(w1t[:, 2 * latent:], hm) + vec_at(4)
        pre_buf[:, span] = pre
        act = (pre * sigmoid(pre)).astype(BF)
        normed, mean, inv = norm_fwd(mm(w2t[...], act) + vec_at(5))
        mean_buf[:, span] = mean
        inv_buf[:, span] = inv
        hi, mid, lo = split3(he.astype(F32) + (normed * vec_at(6) + vec_at(7)))
        add = mm_t(hi, hot) + mm_t(mid, hot) + mm_t(lo, hot)
        for idx, tile in enumerate(tiles):
            agg_buf[tile] += add[:, idx * LANES:(idx + 1) * LANES]

    def backward(sub, whole, slot):
        span, src_hot, tiles, hot = edges_of(sub, whole)
        to = pl.ds(pl.multiple_of(slot * SUB, SUB), SUB)
        both = mm(jnp.concatenate([both_t[t] for t in tiles], axis=1), hot).astype(BF)
        hm_buf[:, to] = both[:latent]
        hot_buf[:, to] = src_hot
        pre = pre_buf[:, span]
        sig = sigmoid(pre)
        act = (pre * sig).astype(BF)
        act_buf[:, to] = act
        inv = inv_buf[:, span]
        normed = (mm(w2t[...], act) + vec_at(5) - mean_buf[:, span]) * inv
        d_norm = mm(node_w1[latent:], both[latent:]) * vec_at(6)
        g_two = norm_bwd(d_norm, normed, inv).astype(BF)
        g2_buf[:, to] = g_two
        g1_buf[:, to] = (mm(w2[...], g_two) * sig * (1.0 + pre * (1.0 - sig))).astype(BF)

    pairs = (live_ref[0] + STEP - 1) // STEP
    per_step = STEP // SUB

    @pl.loop(0, pairs)
    def _(step):
        fit = fit_ref[step] == 1

        @pl.when(fit)
        def _():
            for sub in range(per_step):
                forward(step * per_step + sub, False)

        @pl.when(jnp.logical_not(fit))
        def _():
            @pl.loop(0, per_step)
            def _(sub):
                forward(step * per_step + sub, True)

    hm_buf[...] = turned(node_w1[...])
    act_buf[:, :latent] = turned(node_w2[...])
    for blk in range(mesh_tiles // per_sub):
        tiles = range(blk * per_sub, (blk + 1) * per_sub)
        hm = jnp.concatenate([both_t[t, :latent] for t in tiles], axis=1)
        agg = jnp.concatenate([agg_buf[t].astype(BF) for t in tiles], axis=1)
        pre = mm(hm_buf[:, :latent], hm) + mm(hm_buf[:, latent:], agg) + col(3, 0)
        sig = sigmoid(pre)
        normed, _, inv = norm_fwd(mm(act_buf[:, :latent], (pre * sig).astype(BF)) + col(3, 1))
        out = (hm.astype(F32) + (normed * col(3, 2) + col(3, 3))).astype(BF)
        rows = pl.ds(blk * SUB, SUB)
        mesh_out[rows] = turned(out)
        g_two = norm_bwd(mm_t(eye, cot_ref[rows]) * col(3, 2), normed, inv).astype(BF)
        g_one = (mm(node_w2[...], g_two) * sig * (1.0 + pre * (1.0 - sig))).astype(BF)
        for idx, tile in enumerate(tiles):
            both_t[tile, latent:] = g_one[:, idx * LANES:(idx + 1) * LANES]

    @pl.loop(0, pairs)
    def _(step):
        fit = fit_ref[step] == 1

        @pl.when(fit)
        def _():
            for sub in range(per_step):
                backward(step * per_step + sub, False, sub)

        @pl.when(jnp.logical_not(fit))
        def _():
            @pl.loop(0, per_step)
            def _(sub):
                backward(step * per_step + sub, True, sub)

        w2_out[...] += mm_t(act_buf[...], g2_buf[...])
        g_one = g1_buf[...]
        span = pl.ds(pl.multiple_of(step * STEP, STEP), STEP)
        w1_out[:latent] += mm_t(he_buf[:, span], g_one)
        w1_out[2 * latent:] += mm_t(hm_buf[...], g_one)
        table_out[...] += mm_t(hot_buf[...], g_one)

    hi, mid, lo = split3(table_out[...])
    w1_out[latent:2 * latent] = mm(table_t[...], hi) + mm(table_t[...], mid) + mm(table_t[...], lo)
    w1b = w1[latent:2 * latent]
    table_out[...] = mm_t(hi, w1b) + mm_t(mid, w1b) + mm_t(lo, w1b)


def edge_call(first_tile, fits, live, feats, key_row, mesh_x, below, band, above, small_w, em_w2, mesh_w2, w1, w2,
              node_w1, node_w2, vecs, cot_mesh):
    latent = w2.shape[0]
    edges = key_row.shape[1]
    mesh_rows = cot_mesh.shape[0]
    mesh_tiles = mesh_rows // LANES
    table_rows = below.shape[0] + band.shape[0] + above.shape[0]
    vm = pl.BlockSpec(memory_space=pltpu.VMEM)
    sm = pl.BlockSpec(memory_space=pltpu.SMEM)
    scratch = [((latent, latent), BF), ((latent, 3 * latent), BF), ((latent, latent), BF), ((latent, table_rows), BF),
               ((mesh_tiles, 2 * latent, LANES), BF), ((8, latent, LANES), F32), ((latent, edges), F32), ((latent, edges), BF),
               ((1, edges), F32), ((1, edges), F32), ((mesh_tiles, latent, LANES), F32),
               ((latent, STEP), BF), ((latent, STEP), BF), ((latent, STEP), BF), ((latent, STEP), BF), ((table_rows, STEP), BF)]
    return pl.pallas_call(
        edge_kernel,
        in_specs=[sm] * 3 + [vm] * 15, out_specs=[vm] * 4,
        out_shape=[jax.ShapeDtypeStruct((mesh_rows, latent), BF), jax.ShapeDtypeStruct((3 * latent, latent), F32),
                   jax.ShapeDtypeStruct((latent, latent), F32), jax.ShapeDtypeStruct((table_rows, latent), F32)],
        scratch_shapes=[pltpu.VMEM(shape, dtype) for shape, dtype in scratch],
        compiler_params=pltpu.CompilerParams(vmem_limit_bytes=67043328),
        cost_estimate=pl.CostEstimate(flops=36 * edges * latent * latent, bytes_accessed=20 * 2 ** 20,
                                      transcendentals=3 * edges * latent),
        name="edge_both",
    )(first_tile, fits, live, feats, key_row, mesh_x, below, band, above, small_w, em_w2, mesh_w2, w1, w2,
      node_w1, node_w2, vecs, cot_mesh)


STRIDE = {'z': 32, 'y': 8, 'x': 2}
ORDERS = (('x', 'y', 'z'), ('y', 'z', 'x'), ('z', 'x', 'y'))
DIM = 4


def scatter_kernel(w1_ref, w2_ref, g1_out, g2_out, pair1, pair2, *scratch):
    full = scratch[0:3]
    recv = (scratch[3:6], scratch[6:9], scratch[9:12])
    part = (scratch[12:15], scratch[15:18])
    done1, done2, pair_send, pair_recv, hop_send, hop_recv = scratch[18:]
    me = lax.axis_index('graph')
    core = me % 2
    coord = {name: (me // stride) % DIM for name, stride in STRIDE.items()}
    partner = me + 1 - 2 * core

    def peer(name, hop):
        there = (coord[name] + hop) % DIM
        return there, me + (there - coord[name]) * STRIDE[name]

    barrier = pltpu.get_barrier_semaphore()
    others = [partner] + [peer(name, hop)[1] for name in STRIDE for hop in range(1, DIM)]
    for other in others:
        pl.semaphore_signal(barrier, inc=1, device_id={'graph': other}, device_id_type=MESH)
    pl.semaphore_wait(barrier, len(others))

    half = w1_ref.shape[-1] // 2
    mine = pl.multiple_of(core * half, half)
    theirs = pl.multiple_of((1 - core) * half, half)

    def to_partner(src, dst, slot):
        copy = pltpu.make_async_remote_copy(src_ref=src, dst_ref=dst, send_sem=pair_send.at[slot], recv_sem=pair_recv.at[slot],
                                            device_id={'graph': partner}, device_id_type=MESH)
        copy.start()
        return copy

    first = [to_partner(w1_ref.at[:, :, :, :, pl.ds(theirs, half)], pair1, 0),
             to_partner(w2_ref.at[:, :, :, :, pl.ds(theirs, half)], pair2, 1)]
    first[0].wait()
    quarter = half // 2
    full[0][...] = w1_ref[:, :, :, :, pl.ds(mine, quarter)] + pair1[:, :, :, :, :quarter]
    full[1][...] = w1_ref[:, :, :, :, pl.ds(mine + quarter, quarter)] + pair1[:, :, :, :, quarter:]
    first[1].wait()
    full[2][...] = w2_ref[:, :, :, :, pl.ds(mine, half)] + pair2[...]

    left = [list(STRIDE) for _ in range(3)]
    held = list(full)

    def at(color, name, index):
        pos = left[color].index(name)
        return (slice(None),) * pos + (index,)

    for stage in range(3):
        copies = []
        for color in range(3):
            name = ORDERS[color][stage]
            for hop in range(1, DIM):
                there, device = peer(name, hop)
                copy = pltpu.make_async_remote_copy(
                    src_ref=held[color].at[at(color, name, there)], dst_ref=recv[stage][color].at[hop - 1],
                    send_sem=hop_send.at[stage, color, hop - 1], recv_sem=hop_recv.at[stage, color, hop - 1],
                    device_id={'graph': device}, device_id_type=MESH)
                copy.start()
                copies.append(copy)
        for color in range(3):
            for copy in copies[3 * color:3 * color + 3]:
                copy.wait()
            name = ORDERS[color][stage]
            got = recv[stage][color]
            total = held[color][at(color, name, coord[name])] + got[0] + got[1] + got[2]
            left[color].remove(name)
            if stage < 2:
                part[stage][color][...] = total
                held[color] = part[stage][color]
            elif color == 2:
                done2[core] = total
            else:
                done1[core, :, color * quarter:(color + 1) * quarter] = total

    last = [to_partner(done1.at[core], done1.at[core], 2), to_partner(done2.at[core], done2.at[core], 3)]
    for copy in last:
        copy.wait()
    for done, out in ((done1, g1_out), (done2, g2_out)):
        rows = out.shape[0]
        whole = jnp.concatenate([done[0], done[1]], axis=1)
        out[...] = jnp.where(core == 0, whole[:rows], whole[rows:])


def scatter_call(w1, w2):
    rows1, rows2, cols = w1.shape[-2], w2.shape[-2], w1.shape[-1]
    half, quarter = cols // 2, cols // 4
    tail = ((rows1, quarter), (rows1, quarter), (rows2, half))
    scratch = [pltpu.VMEM((DIM,) * 3 + (rows1, half), F32), pltpu.VMEM((DIM,) * 3 + (rows2, half), F32)]
    scratch += [pltpu.VMEM((DIM,) * 3 + t, F32) for t in tail]
    for stage in range(3):
        scratch += [pltpu.VMEM((3,) + (DIM,) * (2 - stage) + t, F32) for t in tail]
    for stage in range(2):
        scratch += [pltpu.VMEM((DIM,) * (2 - stage) + t, F32) for t in tail]
    scratch += [pltpu.VMEM((2, rows1, half), F32), pltpu.VMEM((2, rows2, half), F32),
                pltpu.SemaphoreType.DMA((4,)), pltpu.SemaphoreType.DMA((4,)),
                pltpu.SemaphoreType.DMA((3, 3, 3)), pltpu.SemaphoreType.DMA((3, 3, 3))]
    vm = pl.BlockSpec(memory_space=pltpu.VMEM)
    return pl.pallas_call(
        scatter_kernel,
        in_specs=[vm, vm], out_specs=[vm, vm],
        out_shape=[jax.ShapeDtypeStruct((rows1 // 2, cols), F32), jax.ShapeDtypeStruct((rows2 // 2, cols), F32)],
        scratch_shapes=scratch,
        compiler_params=pltpu.CompilerParams(collective_id=0, has_side_effects=True, vmem_limit_bytes=40 * 2 ** 20),
        name="weight_scatter",
    )(w1, w2)


def mlp_forward(x_in, w_one, w_two, vec_rows):
    pre_one = jnp.dot(x_in, w_one, preferred_element_type=jnp.float32) + vec_rows[0]
    act_bf = jax.nn.silu(pre_one).astype(jnp.bfloat16)
    pre_two = jnp.dot(act_bf, w_two, preferred_element_type=jnp.float32) + vec_rows[1]
    centred = pre_two - jnp.mean(pre_two, axis=-1, keepdims=True)
    inv_std = lax.rsqrt(jnp.mean(centred * centred, axis=-1, keepdims=True) + NORM_EPS)
    normed = centred * inv_std
    return normed * vec_rows[2] + vec_rows[3], (pre_one, act_bf, normed, inv_std)


def mlp_backward(d_out, w_two, vec_rows, saved_acts):
    pre_one, act_bf, normed, inv_std = saved_acts
    d_norm = d_out * vec_rows[2]
    d_two = inv_std * (d_norm - jnp.mean(d_norm, axis=-1, keepdims=True)
                       - normed * jnp.mean(d_norm * normed, axis=-1, keepdims=True))
    g_two = d_two.astype(jnp.bfloat16)
    d_act = jnp.einsum('nj,kj->nk', g_two, w_two, preferred_element_type=jnp.float32)
    sig_pre = jax.nn.sigmoid(pre_one)
    d_one = d_act * sig_pre * (1.0 + pre_one * (1.0 - sig_pre))
    return d_one.astype(jnp.bfloat16), g_two


def solution(mesh):
    groups = mesh.shape['graph']
    row_spec = P(('batch', 'graph'), None)
    flat_spec = P(('batch', 'graph'))
    rep_spec = P(None, None)
    down_perm = [(src_dev, src_dev - 1) for src_dev in range(1, groups)]
    up_perm = [(src_dev, src_dev + 1) for src_dev in range(groups - 1)]

    def device_step(grid_in, mesh_in, edge_in, edge_src, edge_dst, edge_mask, grid_w1, grid_w2, grid_vec,
                    mesh_w1, mesh_w2, mesh_vec, embed_w1, embed_w2, embed_vec, edge_w1, edge_w2, edge_vec,
                    node_w1, node_w2, node_vec, post_w1, post_w2, post_vec, cot_mesh, cot_grid):
        band_rows = grid_in.shape[0]
        halo_rows = band_rows // 4
        latent = grid_w2.shape[1]
        mesh_rows = mesh_in.shape[0]
        edges = edge_in.shape[0]
        mesh_tiles = mesh_rows // LANES
        band_index = lax.axis_index('graph')

        grid_y, grid_saved = mlp_forward(grid_in.astype(BF), grid_w1, grid_w2, grid_vec)
        grid_h = grid_y.astype(BF)
        from_above = lax.ppermute(grid_h[:halo_rows], 'graph', down_perm)
        from_below = lax.ppermute(grid_h[band_rows - halo_rows:], 'graph', up_perm)

        local_src = edge_src - (band_index * band_rows - halo_rows)
        real = edge_mask != 0
        key = jnp.where(real, edge_dst * 2 ** KEY_BITS + local_src, mesh_rows * 2 ** KEY_BITS)
        feat_t = edge_in.T
        key, f0, f1, f2, f3 = lax.sort((key, feat_t[0], feat_t[1], feat_t[2], feat_t[3]), num_keys=1, is_stable=False)
        zero_row = jnp.zeros_like(f0)
        feats = jnp.stack([f0, f1, f2, f3, zero_row, zero_row, zero_row, zero_row])
        live = jnp.sum(real.astype(jnp.int32)).reshape(1)
        dst_sorted = (key >> KEY_BITS).reshape(-1, SUB)
        low = jnp.min(dst_sorted, axis=1)
        high = jnp.max(jnp.where(dst_sorted < mesh_rows, dst_sorted, 0), axis=1)
        first_tile = jnp.minimum(low // LANES, mesh_tiles - 2)
        fits = ((high - first_tile * LANES) < 2 * LANES).reshape(-1, STEP // SUB)
        fits = jnp.all(fits, axis=1).astype(jnp.int32)
        key_row = key.reshape(1, edges)
        mesh_x = jnp.pad(mesh_in.T, ((0, 8 - mesh_in.shape[1]), (0, 0)))
        small_w = jnp.concatenate([jnp.pad(embed_w1, ((0, 8 - embed_w1.shape[0]), (0, 0))),
                                   jnp.pad(mesh_w1, ((0, 8 - mesh_w1.shape[0]), (0, 0)))])
        vecs = jnp.concatenate([embed_vec, mesh_vec, edge_vec, node_vec])
        mesh_out, w1_part, w2_part, table_grad = edge_call(
            first_tile, fits, live, feats, key_row, mesh_x, from_below, grid_h, from_above, small_w, embed_w2, mesh_w2,
            edge_w1, edge_w2, node_w1, node_w2, vecs, cot_mesh)

        chips = (DIM, DIM, DIM)
        w1_grad, w2_grad = scatter_call(w1_part.reshape(chips + (-1, latent)), w2_part.reshape(chips + (-1, latent)))

        tail_grad = lax.ppermute(table_grad[:halo_rows], 'graph', down_perm)
        head_grad = lax.ppermute(table_grad[band_rows + halo_rows:], 'graph', up_perm)
        post_y, post_saved = mlp_forward(grid_h, post_w1, post_w2, post_vec)
        grid_out = (grid_h.astype(F32) + post_y).astype(BF)
        post_g1 = mlp_backward(cot_grid.astype(F32), post_w2, post_vec, post_saved)[0]
        grid_cot = cot_grid.astype(F32) + jnp.einsum('nj,kj->nk', post_g1, post_w1, preferred_element_type=F32)
        edge_part = table_grad[halo_rows:band_rows + halo_rows] + jnp.concatenate(
            [head_grad, jnp.zeros((band_rows - 2 * halo_rows, latent), F32), tail_grad], axis=0)
        grid_g1 = mlp_backward(grid_cot + edge_part, grid_w2, grid_vec, grid_saved)[0]
        grid_grad = jnp.einsum('nj,kj->nk', grid_g1, grid_w1, preferred_element_type=F32)
        return mesh_out, grid_out, grid_grad, w1_grad, w2_grad

    in_specs = (row_spec, row_spec, row_spec, flat_spec, flat_spec, flat_spec) + (rep_spec,) * 18 + (row_spec, row_spec)
    return jax.shard_map(device_step, mesh=mesh, in_specs=in_specs, out_specs=(row_spec,) * 5, check_vma=False)
```

```python
import functools

import jax
import jax.numpy as jnp
from jax import lax
from jax.experimental import pallas as pl
from jax.experimental.pallas import tpu as pltpu
from jax.sharding import PartitionSpec as P

NORM_EPS = 1e-5
LANES = 128
SUB = 512
STEP = 1024
KEY_BITS = 10
BF = jnp.bfloat16
F32 = jnp.float32
MESH = pl.DeviceIdType.MESH


def mm(lhs, rhs):
    return jnp.dot(lhs, rhs, preferred_element_type=F32)


def mm_t(lhs, rhs):
    return lax.dot_general(lhs, rhs, (((1,), (1,)), ((), ())), preferred_element_type=F32)


def split3(val):
    hi = val.astype(BF)
    rest = val - hi.astype(F32)
    mid = rest.astype(BF)
    lo = (rest - mid.astype(F32)).astype(BF)
    return hi, mid, lo


def sigmoid(val):
    return 0.5 * jnp.tanh(0.5 * val) + 0.5


def lanes_of(col, width):
    return jnp.concatenate([col] * (width // LANES), axis=1)


def one_hot(ids_row, first, rows):
    row_ids = lax.broadcasted_iota(jnp.int32, (rows, ids_row.shape[1]), 0) + first
    return jnp.where(row_ids == ids_row, 1.0, 0.0).astype(BF)


def norm_fwd(val):
    mean = jnp.mean(val, axis=0, keepdims=True)
    centred = val - mean
    inv = lax.rsqrt(jnp.mean(centred * centred, axis=0, keepdims=True) + NORM_EPS)
    return centred * inv, mean, inv


def norm_bwd(d_norm, normed, inv):
    return inv * (d_norm - jnp.mean(d_norm, axis=0, keepdims=True)
                  - normed * jnp.mean(d_norm * normed, axis=0, keepdims=True))


def edge_kernel(first_ref, fit_ref, live_ref, feat_ref, key_ref, mesh_x, below, band, above, small_w, em_w2, mesh_w2,
                w1, w2, node_w1, node_w2, vecs, cot_ref, mesh_out, w1_out, w2_out, table_out,
                em_w2t, w1t, w2t, table_t, both_t, vec_b, pre_buf, he_buf, mean_buf, inv_buf, agg_buf,
                g1_buf, g2_buf, act_buf, hm_buf, hot_buf):
    latent = w2.shape[0]
    table_rows = table_t.shape[1]
    mesh_tiles = both_t.shape[0]
    per_sub = SUB // LANES
    eye = one_hot(lax.broadcasted_iota(jnp.int32, (1, latent), 1), 0, latent)
    turned = lambda val: mm_t(eye, val).astype(BF)

    em_w2t[...] = turned(em_w2[...])
    w2t[...] = turned(w2[...])
    for part in range(3):
        w1t[:, part * latent:(part + 1) * latent] = turned(w1[part * latent:(part + 1) * latent])
    at = 0
    for piece in (below, band, above):
        rows = piece.shape[0]
        table_t[:, at:at + rows] = turned(piece[...])
        at += rows
    cols = jnp.transpose(vecs[...])
    col = lambda mlp, row: cols[:, 4 * mlp + row:4 * mlp + row + 1]
    for row in range(4):
        vec_b[row] = jnp.broadcast_to(col(0, row), (latent, LANES))
        vec_b[4 + row] = jnp.broadcast_to(col(2, row), (latent, LANES))
    small_t = turned(small_w[...])
    agg_buf[...] = jnp.zeros_like(agg_buf)
    w1_out[...] = jnp.zeros_like(w1_out)
    w2_out[...] = jnp.zeros_like(w2_out)
    table_out[...] = jnp.zeros_like(table_out)

    mesh_w2t = turned(mesh_w2[...])
    for blk in range(mesh_tiles // per_sub):
        pre = mm(small_t[:, 8:], mesh_x[:, blk * SUB:(blk + 1) * SUB].astype(BF)) + col(1, 0)
        act = (pre * sigmoid(pre)).astype(BF)
        normed, _, _ = norm_fwd(mm(mesh_w2t, act) + col(1, 1))
        hm = (normed * col(1, 2) + col(1, 3)).astype(BF)
        for idx in range(per_sub):
            both_t[blk * per_sub + idx, :latent] = hm[:, idx * LANES:(idx + 1) * LANES]

    vec_at = lambda row: lanes_of(vec_b[row], SUB)

    def edges_of(sub, whole):
        span = pl.ds(pl.multiple_of(sub * SUB, SUB), SUB)
        key = key_ref[:, span]
        dst = key >> KEY_BITS
        if whole:
            tiles = list(range(mesh_tiles))
            hot = one_hot(dst, 0, mesh_tiles * LANES)
        else:
            first = first_ref[sub]
            tiles = [first, first + 1]
            hot = one_hot(dst, first * LANES, 2 * LANES)
        return span, one_hot(key & (2 ** KEY_BITS - 1), 0, table_rows), tiles, hot

    def forward(sub, whole):
        span, src_hot, tiles, hot = edges_of(sub, whole)
        pre = mm(small_t[:, :8], feat_ref[:, span].astype(BF)) + vec_at(0)
        act = (pre * sigmoid(pre)).astype(BF)
        normed, _, _ = norm_fwd(mm(em_w2t[...], act) + vec_at(1))
        he = (normed * vec_at(2) + vec_at(3)).astype(BF)
        he_buf[:, span] = he
        hg = mm(table_t[...], src_hot).astype(BF)
        hm = mm(jnp.concatenate([both_t[t, :latent] for t in tiles], axis=1), hot).astype(BF)
        pre = mm(w1t[:, :latent], he) + mm(w1t[:, latent:2 * latent], hg) + mm(w1t[:, 2 * latent:], hm) + vec_at(4)
        pre_buf[:, span] = pre
        act = (pre * sigmoid(pre)).astype(BF)
        normed, mean, inv = norm_fwd(mm(w2t[...], act) + vec_at(5))
        mean_buf[:, span] = mean
        inv_buf[:, span] = inv
        hi, mid, lo = split3(he.astype(F32) + (normed * vec_at(6) + vec_at(7)))
        add = mm_t(hi, hot) + mm_t(mid, hot) + mm_t(lo, hot)
        for idx, tile in enumerate(tiles):
            agg_buf[tile] += add[:, idx * LANES:(idx + 1) * LANES]

    def backward(sub, whole, slot):
        span, src_hot, tiles, hot = edges_of(sub, whole)
        to = pl.ds(pl.multiple_of(slot * SUB, SUB), SUB)
        both = mm(jnp.concatenate([both_t[t] for t in tiles], axis=1), hot).astype(BF)
        hm_buf[:, to] = both[:latent]
        hot_buf[:, to] = src_hot
        pre = pre_buf[:, span]
        sig = sigmoid(pre)
        act = (pre * sig).astype(BF)
        act_buf[:, to] = act
        inv = inv_buf[:, span]
        normed = (mm(w2t[...], act) + vec_at(5) - mean_buf[:, span]) * inv
        d_norm = mm(node_w1[latent:], both[latent:]) * vec_at(6)
        g_two = norm_bwd(d_norm, normed, inv).astype(BF)
        g2_buf[:, to] = g_two
        g1_buf[:, to] = (mm(w2[...], g_two) * sig * (1.0 + pre * (1.0 - sig))).astype(BF)

    pairs = (live_ref[0] + STEP - 1) // STEP
    per_step = STEP // SUB

    @pl.loop(0, pairs)
    def _(step):
        fit = fit_ref[step] == 1

        @pl.when(fit)
        def _():
            for sub in range(per_step):
                forward(step * per_step + sub, False)

        @pl.when(jnp.logical_not(fit))
        def _():
            @pl.loop(0, per_step)
            def _(sub):
                forward(step * per_step + sub, True)

    hm_buf[...] = turned(node_w1[...])
    act_buf[:, :latent] = turned(node_w2[...])
    for blk in range(mesh_tiles // per_sub):
        tiles = range(blk * per_sub, (blk + 1) * per_sub)
        hm = jnp.concatenate([both_t[t, :latent] for t in tiles], axis=1)
        agg = jnp.concatenate([agg_buf[t].astype(BF) for t in tiles], axis=1)
        pre = mm(hm_buf[:, :latent], hm) + mm(hm_buf[:, latent:], agg) + col(3, 0)
        sig = sigmoid(pre)
        normed, _, inv = norm_fwd(mm(act_buf[:, :latent], (pre * sig).astype(BF)) + col(3, 1))
        out = (hm.astype(F32) + (normed * col(3, 2) + col(3, 3))).astype(BF)
        rows = pl.ds(blk * SUB, SUB)
        mesh_out[rows] = turned(out)
        g_two = norm_bwd(mm_t(eye, cot_ref[rows]) * col(3, 2), normed, inv).astype(BF)
        g_one = (mm(node_w2[...], g_two) * sig * (1.0 + pre * (1.0 - sig))).astype(BF)
        for idx, tile in enumerate(tiles):
            both_t[tile, latent:] = g_one[:, idx * LANES:(idx + 1) * LANES]

    @pl.loop(0, pairs)
    def _(step):
        fit = fit_ref[step] == 1

        @pl.when(fit)
        def _():
            for sub in range(per_step):
                backward(step * per_step + sub, False, sub)

        @pl.when(jnp.logical_not(fit))
        def _():
            @pl.loop(0, per_step)
            def _(sub):
                backward(step * per_step + sub, True, sub)

        w2_out[...] += mm_t(act_buf[...], g2_buf[...])
        g_one = g1_buf[...]
        span = pl.ds(pl.multiple_of(step * STEP, STEP), STEP)
        w1_out[:latent] += mm_t(he_buf[:, span], g_one)
        w1_out[2 * latent:] += mm_t(hm_buf[...], g_one)
        table_out[...] += mm_t(hot_buf[...], g_one)

    hi, mid, lo = split3(table_out[...])
    w1_out[latent:2 * latent] = mm(table_t[...], hi) + mm(table_t[...], mid) + mm(table_t[...], lo)
    w1b = w1[latent:2 * latent]
    table_out[...] = mm_t(hi, w1b) + mm_t(mid, w1b) + mm_t(lo, w1b)


def edge_call(first_tile, fits, live, feats, key_row, mesh_x, below, band, above, small_w, em_w2, mesh_w2, w1, w2,
              node_w1, node_w2, vecs, cot_mesh):
    latent = w2.shape[0]
    edges = key_row.shape[1]
    mesh_rows = cot_mesh.shape[0]
    mesh_tiles = mesh_rows // LANES
    table_rows = below.shape[0] + band.shape[0] + above.shape[0]
    vm = pl.BlockSpec(memory_space=pltpu.VMEM)
    sm = pl.BlockSpec(memory_space=pltpu.SMEM)
    scratch = [((latent, latent), BF), ((latent, 3 * latent), BF), ((latent, latent), BF), ((latent, table_rows), BF),
               ((mesh_tiles, 2 * latent, LANES), BF), ((8, latent, LANES), F32), ((latent, edges), F32), ((latent, edges), BF),
               ((1, edges), F32), ((1, edges), F32), ((mesh_tiles, latent, LANES), F32),
               ((latent, STEP), BF), ((latent, STEP), BF), ((latent, STEP), BF), ((latent, STEP), BF), ((table_rows, STEP), BF)]
    return pl.pallas_call(
        edge_kernel,
        in_specs=[sm] * 3 + [vm] * 15, out_specs=[vm] * 4,
        out_shape=[jax.ShapeDtypeStruct((mesh_rows, latent), BF), jax.ShapeDtypeStruct((3 * latent, latent), F32),
                   jax.ShapeDtypeStruct((latent, latent), F32), jax.ShapeDtypeStruct((table_rows, latent), F32)],
        scratch_shapes=[pltpu.VMEM(shape, dtype) for shape, dtype in scratch],
        compiler_params=pltpu.CompilerParams(vmem_limit_bytes=67043328),
        cost_estimate=pl.CostEstimate(flops=36 * edges * latent * latent, bytes_accessed=20 * 2 ** 20,
                                      transcendentals=3 * edges * latent),
        name="edge_both",
    )(first_tile, fits, live, feats, key_row, mesh_x, below, band, above, small_w, em_w2, mesh_w2, w1, w2,
      node_w1, node_w2, vecs, cot_mesh)


STRIDE = {'z': 32, 'y': 8, 'x': 2}
ORDERS = (('x', 'y', 'z'), ('y', 'z', 'x'), ('z', 'x', 'y'))
DIM = 4


def row_norm_bwd(d_norm, normed, inv):
    return inv * (d_norm - jnp.mean(d_norm, axis=1, keepdims=True)
                  - normed * jnp.mean(d_norm * normed, axis=1, keepdims=True))


def finish_kernel(groups, w1_ref, w2_ref, table_ref, band_ref, pre_ref, norm_ref, inv_ref, grid_w1, grid_w2, grid_vec,
                  post_w1, post_w2, post_vec, cot_ref, grid_out, grid_grad, g1_out, g2_out, head_buf, tail_buf, cot_buf,
                  pair1, pair2, *scratch):
    full = scratch[0:3]
    recv = (scratch[3:6], scratch[6:9], scratch[9:12])
    part = (scratch[12:15], scratch[15:18])
    done1, done2, pair_send, pair_recv, hop_send, hop_recv, halo_send, halo_recv = scratch[18:]
    me = lax.axis_index('graph')
    core = me % 2
    coord = {name: (me // stride) % DIM for name, stride in STRIDE.items()}
    partner = me + 1 - 2 * core

    def peer(name, hop):
        there = (coord[name] + hop) % DIM
        return there, me + (there - coord[name]) * STRIDE[name]

    barrier = pltpu.get_barrier_semaphore()
    others = [partner, (me + groups - 1 + 2 * core) % groups]
    others += [peer(name, hop)[1] for name in STRIDE for hop in range(1, DIM)]
    for other in others:
        pl.semaphore_signal(barrier, inc=1, device_id={'graph': other}, device_id_type=MESH)
    pl.semaphore_wait(barrier, len(others))

    half = w1_ref.shape[-1] // 2
    mine = pl.multiple_of(core * half, half)
    theirs = pl.multiple_of((1 - core) * half, half)

    def to_partner(src, dst, slot):
        copy = pltpu.make_async_remote_copy(src_ref=src, dst_ref=dst, send_sem=pair_send.at[slot], recv_sem=pair_recv.at[slot],
                                            device_id={'graph': partner}, device_id_type=MESH)
        copy.start()
        return copy

    first = [to_partner(w1_ref.at[:, :, :, :, pl.ds(theirs, half)], pair1, 0),
             to_partner(w2_ref.at[:, :, :, :, pl.ds(theirs, half)], pair2, 1)]
    halo = head_buf.shape[0]
    rows = band_ref.shape[0]
    halo_copies = []
    for slot, (src, dst, device) in enumerate((
            (table_ref.at[pl.ds(0, halo)], tail_buf, (me + groups - 1) % groups),
            (table_ref.at[pl.ds(halo + rows, halo)], head_buf, (me + 1) % groups))):
        copy = pltpu.make_async_remote_copy(src_ref=src, dst_ref=dst, send_sem=halo_send.at[slot], recv_sem=halo_recv.at[slot],
                                            device_id={'graph': device}, device_id_type=MESH)
        copy.start()
        halo_copies.append(copy)

    band = band_ref[...]
    pre = mm(band, post_w1[...]) + post_vec[0:1]
    sig = sigmoid(pre)
    post_q = mm((pre * sig).astype(BF), post_w2[...]) + post_vec[1:2]
    centred = post_q - jnp.mean(post_q, axis=1, keepdims=True)
    inv = lax.rsqrt(jnp.mean(centred * centred, axis=1, keepdims=True) + NORM_EPS)
    normed = centred * inv
    grid_out[...] = (band.astype(F32) + (normed * post_vec[2:3] + post_vec[3:4])).astype(BF)
    cot = cot_ref[...].astype(F32)
    g_two = row_norm_bwd(cot * post_vec[2:3], normed, inv).astype(BF)
    g_one = (mm_t(g_two, post_w2[...]) * sig * (1.0 + pre * (1.0 - sig))).astype(BF)
    cot_buf[...] = cot + mm_t(g_one, post_w1[...])

    first[0].wait()
    quarter = half // 2
    full[0][...] = w1_ref[:, :, :, :, pl.ds(mine, quarter)] + pair1[:, :, :, :, :quarter]
    full[1][...] = w1_ref[:, :, :, :, pl.ds(mine + quarter, quarter)] + pair1[:, :, :, :, quarter:]
    first[1].wait()
    full[2][...] = w2_ref[:, :, :, :, pl.ds(mine, half)] + pair2[...]

    left = [list(STRIDE) for _ in range(3)]
    held = list(full)

    def at(color, name, index):
        pos = left[color].index(name)
        return (slice(None),) * pos + (index,)

    for stage in range(3):
        copies = []
        for color in range(3):
            name = ORDERS[color][stage]
            for hop in range(1, DIM):
                there, device = peer(name, hop)
                copy = pltpu.make_async_remote_copy(
                    src_ref=held[color].at[at(color, name, there)], dst_ref=recv[stage][color].at[hop - 1],
                    send_sem=hop_send.at[stage, color, hop - 1], recv_sem=hop_recv.at[stage, color, hop - 1],
                    device_id={'graph': device}, device_id_type=MESH)
                copy.start()
                copies.append(copy)
        if stage == 0:
            for copy in halo_copies:
                copy.wait()
            no_halo = jnp.zeros((rows - 2 * halo, head_buf.shape[1]), F32)
            edge_part = table_ref[pl.ds(halo, rows)] + jnp.concatenate(
                [jnp.where(me == 0, 0.0, head_buf[...]), no_halo, jnp.where(me == groups - 1, 0.0, tail_buf[...])], axis=0)
            g_two = row_norm_bwd((cot_buf[...] + edge_part) * grid_vec[2:3], norm_ref[...], inv_ref[...]).astype(BF)
            pre = pre_ref[...]
            sig = sigmoid(pre)
            g_one = (mm_t(g_two, grid_w2[...]) * sig * (1.0 + pre * (1.0 - sig))).astype(BF)
            grid_grad[...] = mm_t(g_one, grid_w1[...])
        for color in range(3):
            for copy in copies[3 * color:3 * color + 3]:
                copy.wait()
            name = ORDERS[color][stage]
            got = recv[stage][color]
            total = held[color][at(color, name, coord[name])] + got[0] + got[1] + got[2]
            left[color].remove(name)
            if stage < 2:
                part[stage][color][...] = total
                held[color] = part[stage][color]
            elif color == 2:
                done2[core] = total
            else:
                done1[core, :, color * quarter:(color + 1) * quarter] = total

    last = [to_partner(done1.at[core], done1.at[core], 2), to_partner(done2.at[core], done2.at[core], 3)]
    for copy in last:
        copy.wait()
    for done, out in ((done1, g1_out), (done2, g2_out)):
        rows = out.shape[0]
        whole = jnp.concatenate([done[0], done[1]], axis=1)
        out[...] = jnp.where(core == 0, whole[:rows], whole[rows:])


def finish_call(groups, w1, w2, table_grad, band, pre, norm, inv, grid_w1, grid_w2, grid_vec, post_w1, post_w2, post_vec, cot):
    rows1, rows2, cols = w1.shape[-2], w2.shape[-2], w1.shape[-1]
    half, quarter = cols // 2, cols // 4
    rows = band.shape[0]
    halo = (table_grad.shape[0] - rows) // 2
    tail = ((rows1, quarter), (rows1, quarter), (rows2, half))
    scratch = [pltpu.VMEM((halo, cols), F32), pltpu.VMEM((halo, cols), F32), pltpu.VMEM((rows, cols), F32)]
    scratch += [pltpu.VMEM((DIM,) * 3 + (rows1, half), F32), pltpu.VMEM((DIM,) * 3 + (rows2, half), F32)]
    scratch += [pltpu.VMEM((DIM,) * 3 + t, F32) for t in tail]
    for stage in range(3):
        scratch += [pltpu.VMEM((3,) + (DIM,) * (2 - stage) + t, F32) for t in tail]
    for stage in range(2):
        scratch += [pltpu.VMEM((DIM,) * (2 - stage) + t, F32) for t in tail]
    scratch += [pltpu.VMEM((2, rows1, half), F32), pltpu.VMEM((2, rows2, half), F32),
                pltpu.SemaphoreType.DMA((4,)), pltpu.SemaphoreType.DMA((4,)),
                pltpu.SemaphoreType.DMA((3, 3, 3)), pltpu.SemaphoreType.DMA((3, 3, 3)),
                pltpu.SemaphoreType.DMA((2,)), pltpu.SemaphoreType.DMA((2,))]
    vm = pl.BlockSpec(memory_space=pltpu.VMEM)
    return pl.pallas_call(
        functools.partial(finish_kernel, groups),
        in_specs=[vm] * 14, out_specs=[vm] * 4,
        out_shape=[jax.ShapeDtypeStruct((rows, cols), BF), jax.ShapeDtypeStruct((rows, grid_w1.shape[0]), F32),
                   jax.ShapeDtypeStruct((rows1 // 2, cols), F32), jax.ShapeDtypeStruct((rows2 // 2, cols), F32)],
        scratch_shapes=scratch,
        compiler_params=pltpu.CompilerParams(collective_id=0, has_side_effects=True, vmem_limit_bytes=48 * 2 ** 20),
        name="finish",
    )(w1, w2, table_grad, band, pre, norm, inv, grid_w1, grid_w2, grid_vec, post_w1, post_w2, post_vec, cot)


def mlp_forward(x_in, w_one, w_two, vec_rows):
    pre_one = jnp.dot(x_in, w_one, preferred_element_type=jnp.float32) + vec_rows[0]
    act_bf = jax.nn.silu(pre_one).astype(jnp.bfloat16)
    pre_two = jnp.dot(act_bf, w_two, preferred_element_type=jnp.float32) + vec_rows[1]
    centred = pre_two - jnp.mean(pre_two, axis=-1, keepdims=True)
    inv_std = lax.rsqrt(jnp.mean(centred * centred, axis=-1, keepdims=True) + NORM_EPS)
    normed = centred * inv_std
    return normed * vec_rows[2] + vec_rows[3], (pre_one, act_bf, normed, inv_std)


def solution(mesh):
    groups = mesh.shape['graph']
    row_spec = P(('batch', 'graph'), None)
    flat_spec = P(('batch', 'graph'))
    rep_spec = P(None, None)
    down_perm = [(src_dev, src_dev - 1) for src_dev in range(1, groups)]
    up_perm = [(src_dev, src_dev + 1) for src_dev in range(groups - 1)]

    def device_step(grid_in, mesh_in, edge_in, edge_src, edge_dst, edge_mask, grid_w1, grid_w2, grid_vec,
                    mesh_w1, mesh_w2, mesh_vec, embed_w1, embed_w2, embed_vec, edge_w1, edge_w2, edge_vec,
                    node_w1, node_w2, node_vec, post_w1, post_w2, post_vec, cot_mesh, cot_grid):
        band_rows = grid_in.shape[0]
        halo_rows = band_rows // 4
        latent = grid_w2.shape[1]
        mesh_rows = mesh_in.shape[0]
        edges = edge_in.shape[0]
        mesh_tiles = mesh_rows // LANES
        band_index = lax.axis_index('graph')

        grid_y, grid_saved = mlp_forward(grid_in.astype(BF), grid_w1, grid_w2, grid_vec)
        grid_h = grid_y.astype(BF)
        from_above = lax.ppermute(grid_h[:halo_rows], 'graph', down_perm)
        from_below = lax.ppermute(grid_h[band_rows - halo_rows:], 'graph', up_perm)

        local_src = edge_src - (band_index * band_rows - halo_rows)
        real = edge_mask != 0
        key = jnp.where(real, edge_dst * 2 ** KEY_BITS + local_src, mesh_rows * 2 ** KEY_BITS)
        feat_t = edge_in.T
        key, f0, f1, f2, f3 = lax.sort((key, feat_t[0], feat_t[1], feat_t[2], feat_t[3]), num_keys=1, is_stable=False)
        zero_row = jnp.zeros_like(f0)
        feats = jnp.stack([f0, f1, f2, f3, zero_row, zero_row, zero_row, zero_row])
        live = jnp.sum(real.astype(jnp.int32)).reshape(1)
        dst_sorted = (key >> KEY_BITS).reshape(-1, SUB)
        low = jnp.min(dst_sorted, axis=1)
        high = jnp.max(jnp.where(dst_sorted < mesh_rows, dst_sorted, 0), axis=1)
        first_tile = jnp.minimum(low // LANES, mesh_tiles - 2)
        fits = ((high - first_tile * LANES) < 2 * LANES).reshape(-1, STEP // SUB)
        fits = jnp.all(fits, axis=1).astype(jnp.int32)
        key_row = key.reshape(1, edges)
        mesh_x = jnp.pad(mesh_in.T, ((0, 8 - mesh_in.shape[1]), (0, 0)))
        small_w = jnp.concatenate([jnp.pad(embed_w1, ((0, 8 - embed_w1.shape[0]), (0, 0))),
                                   jnp.pad(mesh_w1, ((0, 8 - mesh_w1.shape[0]), (0, 0)))])
        vecs = jnp.concatenate([embed_vec, mesh_vec, edge_vec, node_vec])
        mesh_out, w1_part, w2_part, table_grad = edge_call(
            first_tile, fits, live, feats, key_row, mesh_x, from_below, grid_h, from_above, small_w, embed_w2, mesh_w2,
            edge_w1, edge_w2, node_w1, node_w2, vecs, cot_mesh)

        chips = (DIM, DIM, DIM)
        grid_pre, _, grid_norm, grid_inv = grid_saved
        grid_out, grid_grad, w1_grad, w2_grad = finish_call(
            groups, w1_part.reshape(chips + (-1, latent)), w2_part.reshape(chips + (-1, latent)), table_grad, grid_h,
            grid_pre, grid_norm, grid_inv, grid_w1, grid_w2, grid_vec, post_w1, post_w2, post_vec, cot_grid)
        return mesh_out, grid_out, grid_grad, w1_grad, w2_grad

    in_specs = (row_spec, row_spec, row_spec, flat_spec, flat_spec, flat_spec) + (rep_spec,) * 18 + (row_spec, row_spec)
    return jax.shard_map(device_step, mesh=mesh, in_specs=in_specs, out_specs=(row_spec,) * 5, check_vma=False)
```

```python
import functools

import jax
import jax.numpy as jnp
from jax import lax
from jax.experimental import pallas as pl
from jax.experimental.pallas import tpu as pltpu
from jax.sharding import PartitionSpec as P

NORM_EPS = 1e-5
LANES = 128
SUB = 512
STEP = 1024
ITEM_BASE = 16
KEY_BITS = 10
BF = jnp.bfloat16
F32 = jnp.float32
MESH = pl.DeviceIdType.MESH


def mm(lhs, rhs):
    return jnp.dot(lhs, rhs, preferred_element_type=F32)


def mm_t(lhs, rhs):
    return lax.dot_general(lhs, rhs, (((1,), (1,)), ((), ())), preferred_element_type=F32)


def split3(val):
    hi = val.astype(BF)
    rest = val - hi.astype(F32)
    mid = rest.astype(BF)
    lo = (rest - mid.astype(F32)).astype(BF)
    return hi, mid, lo


def sigmoid(val):
    return 0.5 * jnp.tanh(0.5 * val) + 0.5


def lanes_of(col, width):
    return jnp.concatenate([col] * (width // LANES), axis=1)


def one_hot(ids_row, first, rows):
    row_ids = lax.broadcasted_iota(jnp.int32, (rows, ids_row.shape[1]), 0) + first
    return jnp.where(row_ids == ids_row, 1.0, 0.0).astype(BF)


def norm_fwd(val):
    mean = jnp.mean(val, axis=0, keepdims=True)
    centred = val - mean
    inv = lax.rsqrt(jnp.mean(centred * centred, axis=0, keepdims=True) + NORM_EPS)
    return centred * inv, mean, inv


def norm_bwd(d_norm, normed, inv):
    return inv * (d_norm - jnp.mean(d_norm, axis=0, keepdims=True)
                  - normed * jnp.mean(d_norm * normed, axis=0, keepdims=True))


def edge_kernel(first_ref, span_ref, fit_ref, live_ref, feat_ref, key_ref, mesh_x, below, band, above, small_w, em_w2, mesh_w2,
                w1, w2, node_w1, node_w2, vecs, cot_ref, mesh_out, w1_out, w2_out, table_out,
                em_w2t, w1t, w2t, table_t, hm_t, ng_t, vec_b, pre_buf, he_buf, mean_buf, inv_buf, agg_buf, item_ref, *slots):
    latent = w2.shape[0]
    table_rows = table_t.shape[1]
    mesh_tiles = hm_t.shape[0]
    slot_a, slot_b = slots[:4], slots[4:]
    per_sub = SUB // LANES
    eye = one_hot(lax.broadcasted_iota(jnp.int32, (1, latent), 1), 0, latent)
    turned = lambda val: mm_t(eye, val).astype(BF)

    em_w2t[...] = turned(em_w2[...])
    w2t[...] = turned(w2[...])
    for part in range(3):
        w1t[:, part * latent:(part + 1) * latent] = turned(w1[part * latent:(part + 1) * latent])
    at = 0
    for piece in (below, band, above):
        rows = piece.shape[0]
        table_t[:, at:at + rows] = turned(piece[...])
        at += rows
    cols = jnp.transpose(vecs[...])
    col = lambda mlp, row: cols[:, 4 * mlp + row:4 * mlp + row + 1]
    for row in range(4):
        vec_b[row] = jnp.broadcast_to(col(0, row), (latent, LANES))
        vec_b[4 + row] = jnp.broadcast_to(col(2, row), (latent, LANES))
    small_t = turned(small_w[...])
    agg_buf[...] = jnp.zeros_like(agg_buf)
    w1_out[:latent] = jnp.zeros_like(w2_out)
    w2_out[...] = jnp.zeros_like(w2_out)
    table_out[...] = jnp.zeros_like(table_out)

    mesh_w2t = turned(mesh_w2[...])
    for blk in range(mesh_tiles // per_sub):
        pre = mm(small_t[:, 8:], mesh_x[:, blk * SUB:(blk + 1) * SUB].astype(BF)) + col(1, 0)
        act = (pre * sigmoid(pre)).astype(BF)
        normed, _, _ = norm_fwd(mm(mesh_w2t, act) + col(1, 1))
        hm = (normed * col(1, 2) + col(1, 3)).astype(BF)
        for idx in range(per_sub):
            hm_t[blk * per_sub + idx] = hm[:, idx * LANES:(idx + 1) * LANES]

    vec_at = lambda row: lanes_of(vec_b[row], SUB)

    def edges_of(sub):
        span = pl.ds(pl.multiple_of(sub * SUB, SUB), SUB)
        key = key_ref[:, span]
        return span, one_hot(key & (2 ** KEY_BITS - 1), 0, table_rows), key >> KEY_BITS

    def forward(sub, whole):
        span, src_hot, dst = edges_of(sub)
        if whole:
            tiles = list(range(mesh_tiles))
            hot = one_hot(dst, 0, mesh_tiles * LANES)
        else:
            first = first_ref[sub]
            tiles = [first, first + 1]
            hot = one_hot(dst, first * LANES, 2 * LANES)
        pre = mm(small_t[:, :8], feat_ref[:, span].astype(BF)) + vec_at(0)
        act = (pre * sigmoid(pre)).astype(BF)
        normed, _, _ = norm_fwd(mm(em_w2t[...], act) + vec_at(1))
        he = (normed * vec_at(2) + vec_at(3)).astype(BF)
        he_buf[:, span] = he
        hg = mm(table_t[...], src_hot).astype(BF)
        hm = mm(jnp.concatenate([hm_t[t] for t in tiles], axis=1), hot).astype(BF)
        pre = mm(w1t[:, :latent], he) + mm(w1t[:, latent:2 * latent], hg) + mm(w1t[:, 2 * latent:], hm) + vec_at(4)
        pre_buf[:, span] = pre
        act = (pre * sigmoid(pre)).astype(BF)
        normed, mean, inv = norm_fwd(mm(w2t[...], act) + vec_at(5))
        mean_buf[:, span] = mean
        inv_buf[:, span] = inv
        hi, mid, lo = split3(he.astype(F32) + (normed * vec_at(6) + vec_at(7)))
        add = mm_t(hi, hot) + mm_t(mid, hot) + mm_t(lo, hot)
        for idx, tile in enumerate(tiles):
            agg_buf[tile] += add[:, idx * LANES:(idx + 1) * LANES]

    def backward(item, slot):
        g1_buf, g2_buf, act_buf, hot_buf = slot
        tile = item % ITEM_BASE
        span, src_hot, dst = edges_of(item // ITEM_BASE)
        hot = one_hot(dst, tile * LANES, 2 * LANES)
        hot_buf[...] = src_hot
        node = mm(jnp.concatenate([ng_t[tile], ng_t[tile + 1]], axis=1), hot).astype(BF)
        pre = pre_buf[:, span]
        sig = sigmoid(pre)
        act = (pre * sig).astype(BF)
        act_buf[...] = act
        inv = inv_buf[:, span]
        normed = (mm(w2t[...], act) + vec_at(5) - mean_buf[:, span]) * inv
        d_norm = mm(node_w1[latent:], node) * vec_at(6)
        g_two = norm_bwd(d_norm, normed, inv).astype(BF)
        g2_buf[...] = g_two
        g_one = (mm(w2[...], g_two) * sig * (1.0 + pre * (1.0 - sig))).astype(BF)
        g1_buf[...] = g_one
        add = mm_t(g_one, hot)
        agg_buf[tile] += add[:, :LANES]
        agg_buf[tile + 1] += add[:, LANES:]

    def weight_sums(item, slot):
        g1_buf, g2_buf, act_buf, hot_buf = slot
        span = pl.ds(pl.multiple_of((item // ITEM_BASE) * SUB, SUB), SUB)
        g_one = g1_buf[...]
        w2_out[...] += mm_t(act_buf[...], g2_buf[...])
        w1_out[:latent] += mm_t(he_buf[:, span], g_one)
        table_out[...] += mm_t(hot_buf[...], g_one)

    pairs = jnp.maximum((live_ref[0] + STEP - 1) // STEP, 1)
    per_step = STEP // SUB

    @pl.loop(0, pairs)
    def _(step):
        fit = fit_ref[step] == 1

        @pl.when(fit)
        def _():
            for sub in range(per_step):
                forward(step * per_step + sub, False)

        @pl.when(jnp.logical_not(fit))
        def _():
            @pl.loop(0, per_step)
            def _(sub):
                forward(step * per_step + sub, True)

    node_a, node_b, node_c = slot_a[:3]
    node_a[...] = turned(node_w1[:latent])
    node_b[...] = turned(node_w1[latent:])
    node_c[...] = turned(node_w2[...])
    for blk in range(mesh_tiles // per_sub):
        tiles = range(blk * per_sub, (blk + 1) * per_sub)
        hm = jnp.concatenate([hm_t[t] for t in tiles], axis=1)
        agg = jnp.concatenate([agg_buf[t].astype(BF) for t in tiles], axis=1)
        pre = mm(node_a[...], hm) + mm(node_b[...], agg) + col(3, 0)
        sig = sigmoid(pre)
        normed, _, inv = norm_fwd(mm(node_c[...], (pre * sig).astype(BF)) + col(3, 1))
        out = (hm.astype(F32) + (normed * col(3, 2) + col(3, 3))).astype(BF)
        rows = pl.ds(blk * SUB, SUB)
        mesh_out[rows] = turned(out)
        g_two = norm_bwd(mm_t(eye, cot_ref[rows]) * col(3, 2), normed, inv).astype(BF)
        g_one = (mm(node_w2[...], g_two) * sig * (1.0 + pre * (1.0 - sig))).astype(BF)
        for idx, tile in enumerate(tiles):
            ng_t[tile] = g_one[:, idx * LANES:(idx + 1) * LANES]
    for tile in range(mesh_tiles, ng_t.shape[0]):
        ng_t[tile] = jnp.zeros((latent, LANES), BF)
    agg_buf[...] = jnp.zeros_like(agg_buf)
    for ref in slot_b:
        ref[...] = jnp.zeros_like(ref)

    def list_sub(sub, count):
        def list_tile(step, _):
            item_ref[count + step] = sub * ITEM_BASE + first_ref[sub] + 2 * step
            return 0

        lax.fori_loop(0, span_ref[sub], list_tile, 0)
        return count + span_ref[sub]

    count = lax.fori_loop(0, pairs * per_step, list_sub, 0)
    item_ref[count] = mesh_tiles

    @pl.loop(0, (count + 1) // 2)
    def _(step):
        before, even, odd = item_ref[jnp.maximum(2 * step - 1, 0)], item_ref[2 * step], item_ref[2 * step + 1]
        backward(even, slot_a)
        weight_sums(before, slot_b)
        backward(odd, slot_b)
        weight_sums(even, slot_a)

    weight_sums(item_ref[jnp.maximum(2 * ((count + 1) // 2) - 1, 0)], slot_b)

    pieces = split3(table_out[...])
    w1b = w1[latent:2 * latent]
    w1_out[latent:2 * latent] = sum(mm(table_t[...], piece) for piece in pieces)
    table_out[...] = sum(mm_t(piece, w1b) for piece in pieces)
    for blk in range(mesh_tiles // per_sub):
        tiles = range(blk * per_sub, (blk + 1) * per_sub)
        hm = jnp.concatenate([hm_t[t] for t in tiles], axis=1)
        pieces = split3(jnp.concatenate([agg_buf[t] for t in tiles], axis=1))
        part = sum(mm_t(hm, piece) for piece in pieces)
        if blk:
            w1_out[2 * latent:] += part
        else:
            w1_out[2 * latent:] = part


def edge_call(first_tile, spans, fits, live, feats, key_row, mesh_x, below, band, above, small_w, em_w2, mesh_w2, w1, w2,
              node_w1, node_w2, vecs, cot_mesh):
    latent = w2.shape[0]
    edges = key_row.shape[1]
    mesh_rows = cot_mesh.shape[0]
    mesh_tiles = mesh_rows // LANES
    table_rows = below.shape[0] + band.shape[0] + above.shape[0]
    vm = pl.BlockSpec(memory_space=pltpu.VMEM)
    sm = pl.BlockSpec(memory_space=pltpu.SMEM)
    scratch = [((latent, latent), BF), ((latent, 3 * latent), BF), ((latent, latent), BF), ((latent, table_rows), BF),
               ((mesh_tiles, latent, LANES), BF), ((mesh_tiles + 2, latent, LANES), BF), ((8, latent, LANES), F32), ((latent, edges), F32), ((latent, edges), BF),
               ((1, edges), F32), ((1, edges), F32), ((mesh_tiles + 2, latent, LANES), F32)]
    slot = [pltpu.VMEM((latent, SUB), BF)] * 3 + [pltpu.VMEM((table_rows, SUB), BF)]
    items = edges // SUB * (mesh_tiles // 2 + 1) + 2
    return pl.pallas_call(
        edge_kernel,
        in_specs=[sm] * 4 + [vm] * 15, out_specs=[vm] * 4,
        out_shape=[jax.ShapeDtypeStruct((mesh_rows, latent), BF), jax.ShapeDtypeStruct((3 * latent, latent), F32),
                   jax.ShapeDtypeStruct((latent, latent), F32), jax.ShapeDtypeStruct((table_rows, latent), F32)],
        scratch_shapes=[pltpu.VMEM(shape, dtype) for shape, dtype in scratch] + [pltpu.SMEM((items,), jnp.int32)] + slot + slot,
        compiler_params=pltpu.CompilerParams(vmem_limit_bytes=67043328),
        cost_estimate=pl.CostEstimate(flops=36 * edges * latent * latent, bytes_accessed=20 * 2 ** 20,
                                      transcendentals=3 * edges * latent),
        name="edge_both",
    )(first_tile, spans, fits, live, feats, key_row, mesh_x, below, band, above, small_w, em_w2, mesh_w2, w1, w2,
      node_w1, node_w2, vecs, cot_mesh)


STRIDE = {'z': 32, 'y': 8, 'x': 2}
ORDERS = (('x', 'y', 'z'), ('y', 'z', 'x'), ('z', 'x', 'y'))
DIM = 4


def row_norm_bwd(d_norm, normed, inv):
    return inv * (d_norm - jnp.mean(d_norm, axis=1, keepdims=True)
                  - normed * jnp.mean(d_norm * normed, axis=1, keepdims=True))


def finish_kernel(groups, w1_ref, w2_ref, table_ref, band_ref, pre_ref, norm_ref, inv_ref, grid_w1, grid_w2, grid_vec,
                  post_w1, post_w2, post_vec, cot_ref, grid_out, grid_grad, g1_out, g2_out, head_buf, tail_buf, cot_buf,
                  pair1, pair2, *scratch):
    full = scratch[0:3]
    recv = (scratch[3:6], scratch[6:9], scratch[9:12])
    part = (scratch[12:15], scratch[15:18])
    done1, done2, pair_send, pair_recv, hop_send, hop_recv, halo_send, halo_recv = scratch[18:]
    me = lax.axis_index('graph')
    core = me % 2
    coord = {name: (me // stride) % DIM for name, stride in STRIDE.items()}
    partner = me + 1 - 2 * core

    def peer(name, hop):
        there = (coord[name] + hop) % DIM
        return there, me + (there - coord[name]) * STRIDE[name]

    barrier = pltpu.get_barrier_semaphore()
    others = [partner, (me + groups - 1 + 2 * core) % groups]
    others += [peer(name, hop)[1] for name in STRIDE for hop in range(1, DIM)]
    for other in others:
        pl.semaphore_signal(barrier, inc=1, device_id={'graph': other}, device_id_type=MESH)
    pl.semaphore_wait(barrier, len(others))

    half = w1_ref.shape[-1] // 2
    mine = pl.multiple_of(core * half, half)
    theirs = pl.multiple_of((1 - core) * half, half)

    def to_partner(src, dst, slot):
        copy = pltpu.make_async_remote_copy(src_ref=src, dst_ref=dst, send_sem=pair_send.at[slot], recv_sem=pair_recv.at[slot],
                                            device_id={'graph': partner}, device_id_type=MESH)
        copy.start()
        return copy

    first = [to_partner(w1_ref.at[:, :, :, :, pl.ds(theirs, half)], pair1, 0),
             to_partner(w2_ref.at[:, :, :, :, pl.ds(theirs, half)], pair2, 1)]
    halo = head_buf.shape[0]
    rows = band_ref.shape[0]
    halo_copies = []
    for slot, (src, dst, device) in enumerate((
            (table_ref.at[pl.ds(0, halo)], tail_buf, (me + groups - 1) % groups),
            (table_ref.at[pl.ds(halo + rows, halo)], head_buf, (me + 1) % groups))):
        copy = pltpu.make_async_remote_copy(src_ref=src, dst_ref=dst, send_sem=halo_send.at[slot], recv_sem=halo_recv.at[slot],
                                            device_id={'graph': device}, device_id_type=MESH)
        copy.start()
        halo_copies.append(copy)

    band = band_ref[...]
    pre = mm(band, post_w1[...]) + post_vec[0:1]
    sig = sigmoid(pre)
    post_q = mm((pre * sig).astype(BF), post_w2[...]) + post_vec[1:2]
    centred = post_q - jnp.mean(post_q, axis=1, keepdims=True)
    inv = lax.rsqrt(jnp.mean(centred * centred, axis=1, keepdims=True) + NORM_EPS)
    normed = centred * inv
    grid_out[...] = (band.astype(F32) + (normed * post_vec[2:3] + post_vec[3:4])).astype(BF)
    cot = cot_ref[...].astype(F32)
    g_two = row_norm_bwd(cot * post_vec[2:3], normed, inv).astype(BF)
    g_one = (mm_t(g_two, post_w2[...]) * sig * (1.0 + pre * (1.0 - sig))).astype(BF)
    cot_buf[...] = cot + mm_t(g_one, post_w1[...])

    first[0].wait()
    quarter = half // 2
    full[0][...] = w1_ref[:, :, :, :, pl.ds(mine, quarter)] + pair1[:, :, :, :, :quarter]
    full[1][...] = w1_ref[:, :, :, :, pl.ds(mine + quarter, quarter)] + pair1[:, :, :, :, quarter:]
    first[1].wait()
    full[2][...] = w2_ref[:, :, :, :, pl.ds(mine, half)] + pair2[...]

    left = [list(STRIDE) for _ in range(3)]
    held = list(full)

    def at(color, name, index):
        pos = left[color].index(name)
        return (slice(None),) * pos + (index,)

    for stage in range(3):
        copies = []
        for color in range(3):
            name = ORDERS[color][stage]
            for hop in range(1, DIM):
                there, device = peer(name, hop)
                copy = pltpu.make_async_remote_copy(
                    src_ref=held[color].at[at(color, name, there)], dst_ref=recv[stage][color].at[hop - 1],
                    send_sem=hop_send.at[stage, color, hop - 1], recv_sem=hop_recv.at[stage, color, hop - 1],
                    device_id={'graph': device}, device_id_type=MESH)
                copy.start()
                copies.append(copy)
        if stage == 0:
            for copy in halo_copies:
                copy.wait()
            no_halo = jnp.zeros((rows - 2 * halo, head_buf.shape[1]), F32)
            edge_part = table_ref[pl.ds(halo, rows)] + jnp.concatenate(
                [jnp.where(me == 0, 0.0, head_buf[...]), no_halo, jnp.where(me == groups - 1, 0.0, tail_buf[...])], axis=0)
            g_two = row_norm_bwd((cot_buf[...] + edge_part) * grid_vec[2:3], norm_ref[...], inv_ref[...]).astype(BF)
            pre = pre_ref[...]
            sig = sigmoid(pre)
            g_one = (mm_t(g_two, grid_w2[...]) * sig * (1.0 + pre * (1.0 - sig))).astype(BF)
            grid_grad[...] = mm_t(g_one, grid_w1[...])
        for color in range(3):
            for copy in copies[3 * color:3 * color + 3]:
                copy.wait()
            name = ORDERS[color][stage]
            got = recv[stage][color]
            total = held[color][at(color, name, coord[name])] + got[0] + got[1] + got[2]
            left[color].remove(name)
            if stage < 2:
                part[stage][color][...] = total
                held[color] = part[stage][color]
            elif color == 2:
                done2[core] = total
            else:
                done1[core, :, color * quarter:(color + 1) * quarter] = total

    last = [to_partner(done1.at[core], done1.at[core], 2), to_partner(done2.at[core], done2.at[core], 3)]
    for copy in last:
        copy.wait()
    for done, out in ((done1, g1_out), (done2, g2_out)):
        rows = out.shape[0]
        whole = jnp.concatenate([done[0], done[1]], axis=1)
        out[...] = jnp.where(core == 0, whole[:rows], whole[rows:])


def finish_call(groups, w1, w2, table_grad, band, pre, norm, inv, grid_w1, grid_w2, grid_vec, post_w1, post_w2, post_vec, cot):
    rows1, rows2, cols = w1.shape[-2], w2.shape[-2], w1.shape[-1]
    half, quarter = cols // 2, cols // 4
    rows = band.shape[0]
    halo = (table_grad.shape[0] - rows) // 2
    tail = ((rows1, quarter), (rows1, quarter), (rows2, half))
    scratch = [pltpu.VMEM((halo, cols), F32), pltpu.VMEM((halo, cols), F32), pltpu.VMEM((rows, cols), F32)]
    scratch += [pltpu.VMEM((DIM,) * 3 + (rows1, half), F32), pltpu.VMEM((DIM,) * 3 + (rows2, half), F32)]
    scratch += [pltpu.VMEM((DIM,) * 3 + t, F32) for t in tail]
    for stage in range(3):
        scratch += [pltpu.VMEM((3,) + (DIM,) * (2 - stage) + t, F32) for t in tail]
    for stage in range(2):
        scratch += [pltpu.VMEM((DIM,) * (2 - stage) + t, F32) for t in tail]
    scratch += [pltpu.VMEM((2, rows1, half), F32), pltpu.VMEM((2, rows2, half), F32),
                pltpu.SemaphoreType.DMA((4,)), pltpu.SemaphoreType.DMA((4,)),
                pltpu.SemaphoreType.DMA((3, 3, 3)), pltpu.SemaphoreType.DMA((3, 3, 3)),
                pltpu.SemaphoreType.DMA((2,)), pltpu.SemaphoreType.DMA((2,))]
    vm = pl.BlockSpec(memory_space=pltpu.VMEM)
    return pl.pallas_call(
        functools.partial(finish_kernel, groups),
        in_specs=[vm] * 14, out_specs=[vm] * 4,
        out_shape=[jax.ShapeDtypeStruct((rows, cols), BF), jax.ShapeDtypeStruct((rows, grid_w1.shape[0]), F32),
                   jax.ShapeDtypeStruct((rows1 // 2, cols), F32), jax.ShapeDtypeStruct((rows2 // 2, cols), F32)],
        scratch_shapes=scratch,
        compiler_params=pltpu.CompilerParams(collective_id=0, has_side_effects=True, vmem_limit_bytes=67043328),
        name="finish",
    )(w1, w2, table_grad, band, pre, norm, inv, grid_w1, grid_w2, grid_vec, post_w1, post_w2, post_vec, cot)


def mlp_forward(x_in, w_one, w_two, vec_rows):
    pre_one = jnp.dot(x_in, w_one, preferred_element_type=jnp.float32) + vec_rows[0]
    act_bf = jax.nn.silu(pre_one).astype(jnp.bfloat16)
    pre_two = jnp.dot(act_bf, w_two, preferred_element_type=jnp.float32) + vec_rows[1]
    centred = pre_two - jnp.mean(pre_two, axis=-1, keepdims=True)
    inv_std = lax.rsqrt(jnp.mean(centred * centred, axis=-1, keepdims=True) + NORM_EPS)
    normed = centred * inv_std
    return normed * vec_rows[2] + vec_rows[3], (pre_one, act_bf, normed, inv_std)


def solution(mesh):
    groups = mesh.shape['graph']
    row_spec = P(('batch', 'graph'), None)
    flat_spec = P(('batch', 'graph'))
    rep_spec = P(None, None)
    down_perm = [(src_dev, src_dev - 1) for src_dev in range(1, groups)]
    up_perm = [(src_dev, src_dev + 1) for src_dev in range(groups - 1)]

    def device_step(grid_in, mesh_in, edge_in, edge_src, edge_dst, edge_mask, grid_w1, grid_w2, grid_vec,
                    mesh_w1, mesh_w2, mesh_vec, embed_w1, embed_w2, embed_vec, edge_w1, edge_w2, edge_vec,
                    node_w1, node_w2, node_vec, post_w1, post_w2, post_vec, cot_mesh, cot_grid):
        band_rows = grid_in.shape[0]
        halo_rows = band_rows // 4
        latent = grid_w2.shape[1]
        mesh_rows = mesh_in.shape[0]
        edges = edge_in.shape[0]
        mesh_tiles = mesh_rows // LANES
        band_index = lax.axis_index('graph')

        grid_y, grid_saved = mlp_forward(grid_in.astype(BF), grid_w1, grid_w2, grid_vec)
        grid_h = grid_y.astype(BF)
        from_above = lax.ppermute(grid_h[:halo_rows], 'graph', down_perm)
        from_below = lax.ppermute(grid_h[band_rows - halo_rows:], 'graph', up_perm)

        local_src = edge_src - (band_index * band_rows - halo_rows)
        real = edge_mask != 0
        key = jnp.where(real, edge_dst * 2 ** KEY_BITS + local_src, mesh_rows * 2 ** KEY_BITS)
        feat_t = edge_in.T
        key, f0, f1, f2, f3 = lax.sort((key, feat_t[0], feat_t[1], feat_t[2], feat_t[3]), num_keys=1, is_stable=False)
        zero_row = jnp.zeros_like(f0)
        feats = jnp.stack([f0, f1, f2, f3, zero_row, zero_row, zero_row, zero_row])
        live = jnp.sum(real.astype(jnp.int32)).reshape(1)
        dst_sorted = (key >> KEY_BITS).reshape(-1, SUB)
        low = jnp.min(dst_sorted, axis=1)
        high = jnp.max(jnp.where(dst_sorted < mesh_rows, dst_sorted, 0), axis=1)
        first_tile = jnp.minimum(low // LANES, mesh_tiles - 2)
        fits = ((high - first_tile * LANES) < 2 * LANES).reshape(-1, STEP // SUB)
        fits = jnp.all(fits, axis=1).astype(jnp.int32)
        spans = jnp.maximum(high // LANES - first_tile, 0) // 2 + 1
        key_row = key.reshape(1, edges)
        mesh_x = jnp.pad(mesh_in.T, ((0, 8 - mesh_in.shape[1]), (0, 0)))
        small_w = jnp.concatenate([jnp.pad(embed_w1, ((0, 8 - embed_w1.shape[0]), (0, 0))),
                                   jnp.pad(mesh_w1, ((0, 8 - mesh_w1.shape[0]), (0, 0)))])
        vecs = jnp.concatenate([embed_vec, mesh_vec, edge_vec, node_vec])
        mesh_out, w1_part, w2_part, table_grad = edge_call(
            first_tile, spans, fits, live, feats, key_row, mesh_x, from_below, grid_h, from_above, small_w, embed_w2, mesh_w2,
            edge_w1, edge_w2, node_w1, node_w2, vecs, cot_mesh)

        chips = (DIM, DIM, DIM)
        grid_pre, _, grid_norm, grid_inv = grid_saved
        grid_out, grid_grad, w1_grad, w2_grad = finish_call(
            groups, w1_part.reshape(chips + (-1, latent)), w2_part.reshape(chips + (-1, latent)), table_grad, grid_h,
            grid_pre, grid_norm, grid_inv, grid_w1, grid_w2, grid_vec, post_w1, post_w2, post_vec, cot_grid)
        return mesh_out, grid_out, grid_grad, w1_grad, w2_grad

    in_specs = (row_spec, row_spec, row_spec, flat_spec, flat_spec, flat_spec) + (rep_spec,) * 18 + (row_spec, row_spec)
    return jax.shard_map(device_step, mesh=mesh, in_specs=in_specs, out_specs=(row_spec,) * 5, check_vma=False)
```

```python
import functools

import jax
import jax.numpy as jnp
from jax import lax
from jax.experimental import pallas as pl
from jax.experimental.pallas import tpu as pltpu
from jax.sharding import PartitionSpec as P

NORM_EPS = 1e-5
LANES = 128
SUB = 512
STEP = 1024
ITEM_BASE = 16
KEY_BITS = 10
BF = jnp.bfloat16
F32 = jnp.float32
MESH = pl.DeviceIdType.MESH


def mm(lhs, rhs):
    return jnp.dot(lhs, rhs, preferred_element_type=F32)


def mm_t(lhs, rhs):
    return lax.dot_general(lhs, rhs, (((1,), (1,)), ((), ())), preferred_element_type=F32)


def split3(val):
    hi = val.astype(BF)
    rest = val - hi.astype(F32)
    mid = rest.astype(BF)
    lo = (rest - mid.astype(F32)).astype(BF)
    return hi, mid, lo


def sigmoid(val):
    return 0.5 * jnp.tanh(0.5 * val) + 0.5


def lanes_of(col, width):
    return jnp.concatenate([col] * (width // LANES), axis=1)


def one_hot(ids_row, first, rows):
    row_ids = lax.broadcasted_iota(jnp.int32, (rows, ids_row.shape[1]), 0) + first
    return jnp.where(row_ids == ids_row, 1.0, 0.0).astype(BF)


def norm_fwd(val):
    mean = jnp.mean(val, axis=0, keepdims=True)
    centred = val - mean
    inv = lax.rsqrt(jnp.mean(centred * centred, axis=0, keepdims=True) + NORM_EPS)
    return centred * inv, mean, inv


def norm_bwd(d_norm, normed, inv):
    return inv * (d_norm - jnp.mean(d_norm, axis=0, keepdims=True)
                  - normed * jnp.mean(d_norm * normed, axis=0, keepdims=True))


def edge_kernel(first_ref, span_ref, fit_ref, live_ref, feat_ref, key_ref, mesh_x, below, band, above, small_w, em_w2, mesh_w2,
                w1, w2, node_w1, node_w2, vecs, cot_ref, mesh_out, w1_out, w2_out, table_out,
                em_w2t, w1t, w2t, table_t, hm_t, ng_t, vec_b, pre_buf, he_buf, mean_buf, inv_buf, agg_buf, item_ref, *slots):
    latent = w2.shape[0]
    table_rows = table_t.shape[1]
    mesh_tiles = hm_t.shape[0]
    slot_a, slot_b = slots[:4], slots[4:]
    per_sub = SUB // LANES
    eye = one_hot(lax.broadcasted_iota(jnp.int32, (1, latent), 1), 0, latent)
    turned = lambda val: mm_t(eye, val).astype(BF)

    em_w2t[...] = turned(em_w2[...])
    w2t[...] = turned(w2[...])
    for part in range(3):
        w1t[:, part * latent:(part + 1) * latent] = turned(w1[part * latent:(part + 1) * latent])
    at = 0
    for piece in (below, band, above):
        rows = piece.shape[0]
        table_t[:, at:at + rows] = turned(piece[...])
        at += rows
    cols = jnp.transpose(vecs[...])
    col = lambda mlp, row: cols[:, 4 * mlp + row:4 * mlp + row + 1]
    for row in range(4):
        vec_b[row] = jnp.broadcast_to(col(0, row), (latent, LANES))
        vec_b[4 + row] = jnp.broadcast_to(col(2, row), (latent, LANES))
    small_t = turned(small_w[...])
    agg_buf[...] = jnp.zeros_like(agg_buf)
    w1_out[:latent] = jnp.zeros_like(w2_out)
    w2_out[...] = jnp.zeros_like(w2_out)
    table_out[...] = jnp.zeros_like(table_out)

    mesh_w2t = turned(mesh_w2[...])
    for blk in range(mesh_tiles // per_sub):
        pre = mm(small_t[:, 8:], mesh_x[:, blk * SUB:(blk + 1) * SUB].astype(BF)) + col(1, 0)
        act = (pre * sigmoid(pre)).astype(BF)
        normed, _, _ = norm_fwd(mm(mesh_w2t, act) + col(1, 1))
        hm = (normed * col(1, 2) + col(1, 3)).astype(BF)
        for idx in range(per_sub):
            hm_t[blk * per_sub + idx] = hm[:, idx * LANES:(idx + 1) * LANES]

    vec_at = lambda row: lanes_of(vec_b[row], SUB)

    def edges_of(sub):
        span = pl.ds(pl.multiple_of(sub * SUB, SUB), SUB)
        key = key_ref[:, span]
        return span, one_hot(key & (2 ** KEY_BITS - 1), 0, table_rows), key >> KEY_BITS

    def forward_many(subs, whole):
        st = []
        for sub in subs:
            span, src_hot, dst = edges_of(sub)
            if whole:
                tiles = list(range(mesh_tiles))
                hot = one_hot(dst, 0, mesh_tiles * LANES)
            else:
                first = first_ref[sub]
                tiles = [first, first + 1]
                hot = one_hot(dst, first * LANES, 2 * LANES)
            st.append(dict(span=span, src_hot=src_hot, tiles=tiles, hot=hot))
        for s in st:
            pre = mm(small_t[:, :8], feat_ref[:, s['span']].astype(BF)) + vec_at(0)
            s['act'] = (pre * sigmoid(pre)).astype(BF)
        for s in st:
            s['hg'] = mm(table_t[...], s['src_hot']).astype(BF)
            s['hm'] = mm(jnp.concatenate([hm_t[t] for t in s['tiles']], axis=1), s['hot']).astype(BF)
            normed, _, _ = norm_fwd(mm(em_w2t[...], s['act']) + vec_at(1))
            s['he'] = (normed * vec_at(2) + vec_at(3)).astype(BF)
            he_buf[:, s['span']] = s['he']
        for s in st:
            pre = mm(w1t[:, latent:2 * latent], s['hg']) + mm(w1t[:, 2 * latent:], s['hm']) + mm(w1t[:, :latent], s['he']) + vec_at(4)
            pre_buf[:, s['span']] = pre
            s['act'] = (pre * sigmoid(pre)).astype(BF)
        for s in st:
            normed, mean, inv = norm_fwd(mm(w2t[...], s['act']) + vec_at(5))
            mean_buf[:, s['span']] = mean
            inv_buf[:, s['span']] = inv
            s['p'] = split3(s['he'].astype(F32) + (normed * vec_at(6) + vec_at(7)))
        for s in st:
            hi, mid, lo = s['p']
            both = mm_t(jnp.concatenate([hi, mid, lo], axis=0), s['hot'])
            add = both[:latent] + both[latent:2 * latent] + both[2 * latent:]
            for idx, tile in enumerate(s['tiles']):
                agg_buf[tile] += add[:, idx * LANES:(idx + 1) * LANES]

    def forward(sub, whole):
        forward_many([sub], whole)

    def backward(item, slot):
        g1_buf, g2_buf, act_buf, hot_buf = slot
        tile = item % ITEM_BASE
        span, src_hot, dst = edges_of(item // ITEM_BASE)
        hot = one_hot(dst, tile * LANES, 2 * LANES)
        hot_buf[...] = src_hot
        pre = pre_buf[:, span]
        sig = sigmoid(pre)
        act = (pre * sig).astype(BF)
        act_buf[...] = act
        node = mm(jnp.concatenate([ng_t[tile], ng_t[tile + 1]], axis=1), hot).astype(BF)
        yield
        inv = inv_buf[:, span]
        normed = (mm(w2t[...], act) + vec_at(5) - mean_buf[:, span]) * inv
        d_norm = mm(node_w1[latent:], node) * vec_at(6)
        yield
        g_two = norm_bwd(d_norm, normed, inv).astype(BF)
        g2_buf[...] = g_two
        yield
        g_one = (mm(w2[...], g_two) * sig * (1.0 + pre * (1.0 - sig))).astype(BF)
        g1_buf[...] = g_one
        yield
        add = mm_t(g_one, hot)
        agg_buf[tile] += add[:, :LANES]
        agg_buf[tile + 1] += add[:, LANES:]

    def weight_sums(item, slot):
        g1_buf, g2_buf, act_buf, hot_buf = slot
        span = pl.ds(pl.multiple_of((item // ITEM_BASE) * SUB, SUB), SUB)
        w2_out[...] += mm_t(act_buf[...], g2_buf[...])
        yield
        w1_out[:latent] += mm_t(he_buf[:, span], g1_buf[...])
        yield
        table_out[...] += mm_t(hot_buf[...], g1_buf[...])

    def together(*parts):
        parts = list(parts)
        while parts:
            for part in list(parts):
                if next(part, parts) is parts:
                    parts.remove(part)

    pairs = jnp.maximum((live_ref[0] + STEP - 1) // STEP, 1)
    per_step = STEP // SUB

    @pl.loop(0, pairs)
    def _(step):
        fit = fit_ref[step] == 1

        @pl.when(fit)
        def _():
            forward_many([step * per_step + sub for sub in range(per_step)], False)

        @pl.when(jnp.logical_not(fit))
        def _():
            @pl.loop(0, per_step)
            def _(sub):
                forward(step * per_step + sub, True)

    node_a, node_b, node_c = slot_a[:3]
    node_a[...] = turned(node_w1[:latent])
    node_b[...] = turned(node_w1[latent:])
    node_c[...] = turned(node_w2[...])
    for blk in range(mesh_tiles // per_sub):
        tiles = range(blk * per_sub, (blk + 1) * per_sub)
        hm = jnp.concatenate([hm_t[t] for t in tiles], axis=1)
        agg = jnp.concatenate([agg_buf[t].astype(BF) for t in tiles], axis=1)
        pre = mm(node_a[...], hm) + mm(node_b[...], agg) + col(3, 0)
        sig = sigmoid(pre)
        normed, _, inv = norm_fwd(mm(node_c[...], (pre * sig).astype(BF)) + col(3, 1))
        out = (hm.astype(F32) + (normed * col(3, 2) + col(3, 3))).astype(BF)
        rows = pl.ds(blk * SUB, SUB)
        mesh_out[rows] = turned(out)
        g_two = norm_bwd(mm_t(eye, cot_ref[rows]) * col(3, 2), normed, inv).astype(BF)
        g_one = (mm(node_w2[...], g_two) * sig * (1.0 + pre * (1.0 - sig))).astype(BF)
        for idx, tile in enumerate(tiles):
            ng_t[tile] = g_one[:, idx * LANES:(idx + 1) * LANES]
    for tile in range(mesh_tiles, ng_t.shape[0]):
        ng_t[tile] = jnp.zeros((latent, LANES), BF)
    agg_buf[...] = jnp.zeros_like(agg_buf)
    for ref in slot_b:
        ref[...] = jnp.zeros_like(ref)

    def list_sub(sub, count):
        def list_tile(step, _):
            item_ref[count + step] = sub * ITEM_BASE + first_ref[sub] + 2 * step
            return 0

        lax.fori_loop(0, span_ref[sub], list_tile, 0)
        return count + span_ref[sub]

    count = lax.fori_loop(0, pairs * per_step, list_sub, 0)
    item_ref[count] = mesh_tiles

    @pl.loop(0, (count + 1) // 2)
    def _(step):
        before, even, odd = item_ref[jnp.maximum(2 * step - 1, 0)], item_ref[2 * step], item_ref[2 * step + 1]
        together(backward(even, slot_a), weight_sums(before, slot_b))
        together(backward(odd, slot_b), weight_sums(even, slot_a))

    together(weight_sums(item_ref[jnp.maximum(2 * ((count + 1) // 2) - 1, 0)], slot_b))

    pieces = split3(table_out[...])
    w1b = w1[latent:2 * latent]
    w1_out[latent:2 * latent] = sum(mm(table_t[...], piece) for piece in pieces)
    table_out[...] = sum(mm_t(piece, w1b) for piece in pieces)
    for blk in range(mesh_tiles // per_sub):
        tiles = range(blk * per_sub, (blk + 1) * per_sub)
        hm = jnp.concatenate([hm_t[t] for t in tiles], axis=1)
        pieces = split3(jnp.concatenate([agg_buf[t] for t in tiles], axis=1))
        part = sum(mm_t(hm, piece) for piece in pieces)
        if blk:
            w1_out[2 * latent:] += part
        else:
            w1_out[2 * latent:] = part


def edge_call(first_tile, spans, fits, live, feats, key_row, mesh_x, below, band, above, small_w, em_w2, mesh_w2, w1, w2,
              node_w1, node_w2, vecs, cot_mesh):
    latent = w2.shape[0]
    edges = key_row.shape[1]
    mesh_rows = cot_mesh.shape[0]
    mesh_tiles = mesh_rows // LANES
    table_rows = below.shape[0] + band.shape[0] + above.shape[0]
    vm = pl.BlockSpec(memory_space=pltpu.VMEM)
    sm = pl.BlockSpec(memory_space=pltpu.SMEM)
    scratch = [((latent, latent), BF), ((latent, 3 * latent), BF), ((latent, latent), BF), ((latent, table_rows), BF),
               ((mesh_tiles, latent, LANES), BF), ((mesh_tiles + 2, latent, LANES), BF), ((8, latent, LANES), F32), ((latent, edges), F32), ((latent, edges), BF),
               ((1, edges), F32), ((1, edges), F32), ((mesh_tiles + 2, latent, LANES), F32)]
    slot = [pltpu.VMEM((latent, SUB), BF)] * 3 + [pltpu.VMEM((table_rows, SUB), BF)]
    items = edges // SUB * (mesh_tiles // 2 + 1) + 2
    return pl.pallas_call(
        edge_kernel,
        in_specs=[sm] * 4 + [vm] * 15, out_specs=[vm] * 4,
        out_shape=[jax.ShapeDtypeStruct((mesh_rows, latent), BF), jax.ShapeDtypeStruct((3 * latent, latent), F32),
                   jax.ShapeDtypeStruct((latent, latent), F32), jax.ShapeDtypeStruct((table_rows, latent), F32)],
        scratch_shapes=[pltpu.VMEM(shape, dtype) for shape, dtype in scratch] + [pltpu.SMEM((items,), jnp.int32)] + slot + slot,
        compiler_params=pltpu.CompilerParams(vmem_limit_bytes=67043328),
        cost_estimate=pl.CostEstimate(flops=36 * edges * latent * latent, bytes_accessed=20 * 2 ** 20,
                                      transcendentals=3 * edges * latent),
        name="edge_both",
    )(first_tile, spans, fits, live, feats, key_row, mesh_x, below, band, above, small_w, em_w2, mesh_w2, w1, w2,
      node_w1, node_w2, vecs, cot_mesh)


STRIDE = {'z': 32, 'y': 8, 'x': 2}
ORDERS = (('x', 'y', 'z'), ('y', 'z', 'x'), ('z', 'x', 'y'))
DIM = 4


def row_norm_bwd(d_norm, normed, inv):
    return inv * (d_norm - jnp.mean(d_norm, axis=1, keepdims=True)
                  - normed * jnp.mean(d_norm * normed, axis=1, keepdims=True))


def finish_kernel(groups, w1_ref, w2_ref, table_ref, band_ref, pre_ref, norm_ref, inv_ref, grid_w1, grid_w2, grid_vec,
                  post_w1, post_w2, post_vec, cot_ref, grid_out, grid_grad, g1_out, g2_out, head_buf, tail_buf, cot_buf,
                  pair1, pair2, *scratch):
    full = scratch[0:3]
    recv = (scratch[3:6], scratch[6:9], scratch[9:12])
    part = (scratch[12:15], scratch[15:18])
    done1, done2, pair_send, pair_recv, hop_send, hop_recv, halo_send, halo_recv = scratch[18:]
    me = lax.axis_index('graph')
    core = me % 2
    coord = {name: (me // stride) % DIM for name, stride in STRIDE.items()}
    partner = me + 1 - 2 * core

    def peer(name, hop):
        there = (coord[name] + hop) % DIM
        return there, me + (there - coord[name]) * STRIDE[name]

    barrier = pltpu.get_barrier_semaphore()
    others = [partner, (me + groups - 1 + 2 * core) % groups]
    others += [peer(name, hop)[1] for name in STRIDE for hop in range(1, DIM)]
    for other in others:
        pl.semaphore_signal(barrier, inc=1, device_id={'graph': other}, device_id_type=MESH)
    pl.semaphore_wait(barrier, len(others))

    half = w1_ref.shape[-1] // 2
    mine = pl.multiple_of(core * half, half)
    theirs = pl.multiple_of((1 - core) * half, half)

    def to_partner(src, dst, slot):
        copy = pltpu.make_async_remote_copy(src_ref=src, dst_ref=dst, send_sem=pair_send.at[slot], recv_sem=pair_recv.at[slot],
                                            device_id={'graph': partner}, device_id_type=MESH)
        copy.start()
        return copy

    first = [to_partner(w1_ref.at[:, :, :, :, pl.ds(theirs, half)], pair1, 0),
             to_partner(w2_ref.at[:, :, :, :, pl.ds(theirs, half)], pair2, 1)]
    halo = head_buf.shape[0]
    rows = band_ref.shape[0]
    halo_copies = []
    for slot, (src, dst, device) in enumerate((
            (table_ref.at[pl.ds(0, halo)], tail_buf, (me + groups - 1) % groups),
            (table_ref.at[pl.ds(halo + rows, halo)], head_buf, (me + 1) % groups))):
        copy = pltpu.make_async_remote_copy(src_ref=src, dst_ref=dst, send_sem=halo_send.at[slot], recv_sem=halo_recv.at[slot],
                                            device_id={'graph': device}, device_id_type=MESH)
        copy.start()
        halo_copies.append(copy)

    band = band_ref[...]
    pre = mm(band, post_w1[...]) + post_vec[0:1]
    sig = sigmoid(pre)
    post_q = mm((pre * sig).astype(BF), post_w2[...]) + post_vec[1:2]
    centred = post_q - jnp.mean(post_q, axis=1, keepdims=True)
    inv = lax.rsqrt(jnp.mean(centred * centred, axis=1, keepdims=True) + NORM_EPS)
    normed = centred * inv
    grid_out[...] = (band.astype(F32) + (normed * post_vec[2:3] + post_vec[3:4])).astype(BF)
    cot = cot_ref[...].astype(F32)
    g_two = row_norm_bwd(cot * post_vec[2:3], normed, inv).astype(BF)
    g_one = (mm_t(g_two, post_w2[...]) * sig * (1.0 + pre * (1.0 - sig))).astype(BF)
    cot_buf[...] = cot + mm_t(g_one, post_w1[...])

    first[0].wait()
    quarter = half // 2
    full[0][...] = w1_ref[:, :, :, :, pl.ds(mine, quarter)] + pair1[:, :, :, :, :quarter]
    full[1][...] = w1_ref[:, :, :, :, pl.ds(mine + quarter, quarter)] + pair1[:, :, :, :, quarter:]
    first[1].wait()
    full[2][...] = w2_ref[:, :, :, :, pl.ds(mine, half)] + pair2[...]

    left = [list(STRIDE) for _ in range(3)]
    held = list(full)

    def at(color, name, index):
        pos = left[color].index(name)
        return (slice(None),) * pos + (index,)

    for stage in range(3):
        copies = []
        for color in range(3):
            name = ORDERS[color][stage]
            for hop in range(1, DIM):
                there, device = peer(name, hop)
                copy = pltpu.make_async_remote_copy(
                    src_ref=held[color].at[at(color, name, there)], dst_ref=recv[stage][color].at[hop - 1],
                    send_sem=hop_send.at[stage, color, hop - 1], recv_sem=hop_recv.at[stage, color, hop - 1],
                    device_id={'graph': device}, device_id_type=MESH)
                copy.start()
                copies.append(copy)
        if stage == 0:
            for copy in halo_copies:
                copy.wait()
            no_halo = jnp.zeros((rows - 2 * halo, head_buf.shape[1]), F32)
            edge_part = table_ref[pl.ds(halo, rows)] + jnp.concatenate(
                [jnp.where(me == 0, 0.0, head_buf[...]), no_halo, jnp.where(me == groups - 1, 0.0, tail_buf[...])], axis=0)
            g_two = row_norm_bwd((cot_buf[...] + edge_part) * grid_vec[2:3], norm_ref[...], inv_ref[...]).astype(BF)
            pre = pre_ref[...]
            sig = sigmoid(pre)
            g_one = (mm_t(g_two, grid_w2[...]) * sig * (1.0 + pre * (1.0 - sig))).astype(BF)
            grid_grad[...] = mm_t(g_one, grid_w1[...])
        for color in range(3):
            for copy in copies[3 * color:3 * color + 3]:
                copy.wait()
            name = ORDERS[color][stage]
            got = recv[stage][color]
            total = held[color][at(color, name, coord[name])] + got[0] + got[1] + got[2]
            left[color].remove(name)
            if stage < 2:
                part[stage][color][...] = total
                held[color] = part[stage][color]
            elif color == 2:
                done2[core] = total
            else:
                done1[core, :, color * quarter:(color + 1) * quarter] = total

    last = [to_partner(done1.at[core], done1.at[core], 2), to_partner(done2.at[core], done2.at[core], 3)]
    for copy in last:
        copy.wait()
    for done, out in ((done1, g1_out), (done2, g2_out)):
        rows = out.shape[0]
        whole = jnp.concatenate([done[0], done[1]], axis=1)
        out[...] = jnp.where(core == 0, whole[:rows], whole[rows:])


def finish_call(groups, w1, w2, table_grad, band, pre, norm, inv, grid_w1, grid_w2, grid_vec, post_w1, post_w2, post_vec, cot):
    rows1, rows2, cols = w1.shape[-2], w2.shape[-2], w1.shape[-1]
    half, quarter = cols // 2, cols // 4
    rows = band.shape[0]
    halo = (table_grad.shape[0] - rows) // 2
    tail = ((rows1, quarter), (rows1, quarter), (rows2, half))
    scratch = [pltpu.VMEM((halo, cols), F32), pltpu.VMEM((halo, cols), F32), pltpu.VMEM((rows, cols), F32)]
    scratch += [pltpu.VMEM((DIM,) * 3 + (rows1, half), F32), pltpu.VMEM((DIM,) * 3 + (rows2, half), F32)]
    scratch += [pltpu.VMEM((DIM,) * 3 + t, F32) for t in tail]
    for stage in range(3):
        scratch += [pltpu.VMEM((3,) + (DIM,) * (2 - stage) + t, F32) for t in tail]
    for stage in range(2):
        scratch += [pltpu.VMEM((DIM,) * (2 - stage) + t, F32) for t in tail]
    scratch += [pltpu.VMEM((2, rows1, half), F32), pltpu.VMEM((2, rows2, half), F32),
                pltpu.SemaphoreType.DMA((4,)), pltpu.SemaphoreType.DMA((4,)),
                pltpu.SemaphoreType.DMA((3, 3, 3)), pltpu.SemaphoreType.DMA((3, 3, 3)),
                pltpu.SemaphoreType.DMA((2,)), pltpu.SemaphoreType.DMA((2,))]
    vm = pl.BlockSpec(memory_space=pltpu.VMEM)
    return pl.pallas_call(
        functools.partial(finish_kernel, groups),
        in_specs=[vm] * 14, out_specs=[vm] * 4,
        out_shape=[jax.ShapeDtypeStruct((rows, cols), BF), jax.ShapeDtypeStruct((rows, grid_w1.shape[0]), F32),
                   jax.ShapeDtypeStruct((rows1 // 2, cols), F32), jax.ShapeDtypeStruct((rows2 // 2, cols), F32)],
        scratch_shapes=scratch,
        compiler_params=pltpu.CompilerParams(collective_id=0, has_side_effects=True, vmem_limit_bytes=67043328),
        name="finish",
    )(w1, w2, table_grad, band, pre, norm, inv, grid_w1, grid_w2, grid_vec, post_w1, post_w2, post_vec, cot)


def mlp_forward(x_in, w_one, w_two, vec_rows):
    pre_one = jnp.dot(x_in, w_one, preferred_element_type=jnp.float32) + vec_rows[0]
    act_bf = jax.nn.silu(pre_one).astype(jnp.bfloat16)
    pre_two = jnp.dot(act_bf, w_two, preferred_element_type=jnp.float32) + vec_rows[1]
    centred = pre_two - jnp.mean(pre_two, axis=-1, keepdims=True)
    inv_std = lax.rsqrt(jnp.mean(centred * centred, axis=-1, keepdims=True) + NORM_EPS)
    normed = centred * inv_std
    return normed * vec_rows[2] + vec_rows[3], (pre_one, act_bf, normed, inv_std)


def solution(mesh):
    groups = mesh.shape['graph']
    row_spec = P(('batch', 'graph'), None)
    flat_spec = P(('batch', 'graph'))
    rep_spec = P(None, None)
    down_perm = [(src_dev, src_dev - 1) for src_dev in range(1, groups)]
    up_perm = [(src_dev, src_dev + 1) for src_dev in range(groups - 1)]

    def device_step(grid_in, mesh_in, edge_in, edge_src, edge_dst, edge_mask, grid_w1, grid_w2, grid_vec,
                    mesh_w1, mesh_w2, mesh_vec, embed_w1, embed_w2, embed_vec, edge_w1, edge_w2, edge_vec,
                    node_w1, node_w2, node_vec, post_w1, post_w2, post_vec, cot_mesh, cot_grid):
        band_rows = grid_in.shape[0]
        halo_rows = band_rows // 4
        latent = grid_w2.shape[1]
        mesh_rows = mesh_in.shape[0]
        edges = edge_in.shape[0]
        mesh_tiles = mesh_rows // LANES
        band_index = lax.axis_index('graph')

        grid_y, grid_saved = mlp_forward(grid_in.astype(BF), grid_w1, grid_w2, grid_vec)
        grid_h = grid_y.astype(BF)
        from_above = lax.ppermute(grid_h[:halo_rows], 'graph', down_perm)
        from_below = lax.ppermute(grid_h[band_rows - halo_rows:], 'graph', up_perm)

        local_src = edge_src - (band_index * band_rows - halo_rows)
        real = edge_mask != 0
        key = jnp.where(real, edge_dst * 2 ** KEY_BITS + local_src, mesh_rows * 2 ** KEY_BITS)
        feat_t = edge_in.T
        key, f0, f1, f2, f3 = lax.sort((key, feat_t[0], feat_t[1], feat_t[2], feat_t[3]), num_keys=1, is_stable=False)
        zero_row = jnp.zeros_like(f0)
        feats = jnp.stack([f0, f1, f2, f3, zero_row, zero_row, zero_row, zero_row])
        live = jnp.sum(real.astype(jnp.int32)).reshape(1)
        dst_sorted = (key >> KEY_BITS).reshape(-1, SUB)
        low = jnp.min(dst_sorted, axis=1)
        high = jnp.max(jnp.where(dst_sorted < mesh_rows, dst_sorted, 0), axis=1)
        first_tile = jnp.minimum(low // LANES, mesh_tiles - 2)
        fits = ((high - first_tile * LANES) < 2 * LANES).reshape(-1, STEP // SUB)
        fits = jnp.all(fits, axis=1).astype(jnp.int32)
        spans = jnp.maximum(high // LANES - first_tile, 0) // 2 + 1
        key_row = key.reshape(1, edges)
        mesh_x = jnp.pad(mesh_in.T, ((0, 8 - mesh_in.shape[1]), (0, 0)))
        small_w = jnp.concatenate([jnp.pad(embed_w1, ((0, 8 - embed_w1.shape[0]), (0, 0))),
                                   jnp.pad(mesh_w1, ((0, 8 - mesh_w1.shape[0]), (0, 0)))])
        vecs = jnp.concatenate([embed_vec, mesh_vec, edge_vec, node_vec])
        mesh_out, w1_part, w2_part, table_grad = edge_call(
            first_tile, spans, fits, live, feats, key_row, mesh_x, from_below, grid_h, from_above, small_w, embed_w2, mesh_w2,
            edge_w1, edge_w2, node_w1, node_w2, vecs, cot_mesh)

        chips = (DIM, DIM, DIM)
        grid_pre, _, grid_norm, grid_inv = grid_saved
        grid_out, grid_grad, w1_grad, w2_grad = finish_call(
            groups, w1_part.reshape(chips + (-1, latent)), w2_part.reshape(chips + (-1, latent)), table_grad, grid_h,
            grid_pre, grid_norm, grid_inv, grid_w1, grid_w2, grid_vec, post_w1, post_w2, post_vec, cot_grid)
        return mesh_out, grid_out, grid_grad, w1_grad, w2_grad

    in_specs = (row_spec, row_spec, row_spec, flat_spec, flat_spec, flat_spec) + (rep_spec,) * 18 + (row_spec, row_spec)
    return jax.shard_map(device_step, mesh=mesh, in_specs=in_specs, out_specs=(row_spec,) * 5, check_vma=False)
```

```python
import functools

import jax
import jax.numpy as jnp
from jax import lax
from jax.experimental import pallas as pl
from jax.experimental.pallas import tpu as pltpu
from jax.sharding import PartitionSpec as P

NORM_EPS = 1e-5
LANES = 128
SUB = 512
STEP = 1024
ITEM_BASE = 16
KEY_BITS = 10
BF = jnp.bfloat16
F32 = jnp.float32
MESH = pl.DeviceIdType.MESH


def mm(lhs, rhs):
    return jnp.dot(lhs, rhs, preferred_element_type=F32)


def mm_t(lhs, rhs):
    return lax.dot_general(lhs, rhs, (((1,), (1,)), ((), ())), preferred_element_type=F32)


def split3(val):
    hi = val.astype(BF)
    rest = val - hi.astype(F32)
    mid = rest.astype(BF)
    lo = (rest - mid.astype(F32)).astype(BF)
    return hi, mid, lo


def sigmoid(val):
    return 0.5 * jnp.tanh(0.5 * val) + 0.5


def lanes_of(col, width):
    return jnp.concatenate([col] * (width // LANES), axis=1)


def one_hot(ids_row, first, rows):
    row_ids = lax.broadcasted_iota(jnp.int32, (rows, ids_row.shape[1]), 0) + first
    return jnp.where(row_ids == ids_row, 1.0, 0.0).astype(BF)


def norm_fwd(val):
    mean = jnp.mean(val, axis=0, keepdims=True)
    centred = val - mean
    inv = lax.rsqrt(jnp.mean(centred * centred, axis=0, keepdims=True) + NORM_EPS)
    return centred * inv, mean, inv


def norm_bwd(d_norm, normed, inv):
    return inv * (d_norm - jnp.mean(d_norm, axis=0, keepdims=True)
                  - normed * jnp.mean(d_norm * normed, axis=0, keepdims=True))


def edge_kernel(first_ref, span_ref, fit_ref, live_ref, feat_ref, key_ref, mesh_x, below, band, above, small_w, em_w2, mesh_w2,
                w1, w2, node_w1, node_w2, vecs, cot_ref, mesh_out, w1_out, w2_out, table_out,
                em_w2t, w1t, w2t, table_t, hm_t, ng_t, vec_b, pre_buf, he_buf, mean_buf, inv_buf, agg_buf, item_ref, *slots):
    latent = w2.shape[0]
    table_rows = table_t.shape[1]
    mesh_tiles = hm_t.shape[0]
    slot_a, slot_b = slots[:4], slots[4:]
    per_sub = SUB // LANES
    eye = one_hot(lax.broadcasted_iota(jnp.int32, (1, latent), 1), 0, latent)
    turned = lambda val: mm_t(eye, val).astype(BF)

    em_w2t[...] = turned(em_w2[...])
    w2t[...] = turned(w2[...])
    for part in range(3):
        w1t[:, part * latent:(part + 1) * latent] = turned(w1[part * latent:(part + 1) * latent])
    at = 0
    for piece in (below, band, above):
        rows = piece.shape[0]
        table_t[:, at:at + rows] = turned(piece[...])
        at += rows
    cols = jnp.transpose(vecs[...])
    col = lambda mlp, row: cols[:, 4 * mlp + row:4 * mlp + row + 1]
    for row in range(4):
        vec_b[row] = jnp.broadcast_to(col(0, row), (latent, LANES))
        vec_b[4 + row] = jnp.broadcast_to(col(2, row), (latent, LANES))
    small_t = turned(small_w[...])
    agg_buf[...] = jnp.zeros_like(agg_buf)
    w1_out[:latent] = jnp.zeros_like(w2_out)
    w2_out[...] = jnp.zeros_like(w2_out)
    table_out[...] = jnp.zeros_like(table_out)

    mesh_w2t = turned(mesh_w2[...])
    @pl.loop(0, mesh_tiles // per_sub)
    def _(blk):
        pre = mm(small_t[:, 8:], mesh_x[:, pl.ds(pl.multiple_of(blk * SUB, SUB), SUB)].astype(BF)) + col(1, 0)
        act = (pre * sigmoid(pre)).astype(BF)
        normed, _, _ = norm_fwd(mm(mesh_w2t, act) + col(1, 1))
        hm = (normed * col(1, 2) + col(1, 3)).astype(BF)
        for idx in range(per_sub):
            hm_t[blk * per_sub + idx] = hm[:, idx * LANES:(idx + 1) * LANES]

    vec_at = lambda row: lanes_of(vec_b[row], SUB)

    def edges_of(sub):
        span = pl.ds(pl.multiple_of(sub * SUB, SUB), SUB)
        key = key_ref[:, span]
        return span, one_hot(key & (2 ** KEY_BITS - 1), 0, table_rows), key >> KEY_BITS

    def forward_many(subs, whole):
        st = []
        for sub in subs:
            span, src_hot, dst = edges_of(sub)
            if whole:
                tiles = list(range(mesh_tiles))
                hot = one_hot(dst, 0, mesh_tiles * LANES)
            else:
                first = first_ref[sub]
                tiles = [first, first + 1]
                hot = one_hot(dst, first * LANES, 2 * LANES)
            st.append(dict(span=span, src_hot=src_hot, tiles=tiles, hot=hot))
        for s in st:
            pre = mm(small_t[:, :8], feat_ref[:, s['span']].astype(BF)) + vec_at(0)
            s['act'] = (pre * sigmoid(pre)).astype(BF)
        for s in st:
            s['hg'] = mm(table_t[...], s['src_hot']).astype(BF)
            s['hm'] = mm(jnp.concatenate([hm_t[t] for t in s['tiles']], axis=1), s['hot']).astype(BF)
            normed, _, _ = norm_fwd(mm(em_w2t[...], s['act']) + vec_at(1))
            s['he'] = (normed * vec_at(2) + vec_at(3)).astype(BF)
            he_buf[:, s['span']] = s['he']
        for s in st:
            pre = mm(w1t[:, latent:2 * latent], s['hg']) + mm(w1t[:, 2 * latent:], s['hm']) + mm(w1t[:, :latent], s['he']) + vec_at(4)
            pre_buf[:, s['span']] = pre
            s['act'] = (pre * sigmoid(pre)).astype(BF)
        for s in st:
            normed, mean, inv = norm_fwd(mm(w2t[...], s['act']) + vec_at(5))
            mean_buf[:, s['span']] = mean
            inv_buf[:, s['span']] = inv
            s['p'] = split3(s['he'].astype(F32) + (normed * vec_at(6) + vec_at(7)))
        for s in st:
            hi, mid, lo = s['p']
            both = mm_t(jnp.concatenate([hi, mid, lo], axis=0), s['hot'])
            add = both[:latent] + both[latent:2 * latent] + both[2 * latent:]
            for idx, tile in enumerate(s['tiles']):
                agg_buf[tile] += add[:, idx * LANES:(idx + 1) * LANES]

    def forward(sub, whole):
        forward_many([sub], whole)

    def backward(item, slot):
        g1_buf, g2_buf, act_buf, hot_buf = slot
        tile = item % ITEM_BASE
        span, src_hot, dst = edges_of(item // ITEM_BASE)
        hot = one_hot(dst, tile * LANES, 2 * LANES)
        hot_buf[...] = src_hot
        pre = pre_buf[:, span]
        sig = sigmoid(pre)
        act = (pre * sig).astype(BF)
        act_buf[...] = act
        node = mm(jnp.concatenate([ng_t[tile], ng_t[tile + 1]], axis=1), hot).astype(BF)
        yield
        inv = inv_buf[:, span]
        normed = (mm(w2t[...], act) + vec_at(5) - mean_buf[:, span]) * inv
        d_norm = mm(node_w1[latent:], node) * vec_at(6)
        yield
        g_two = norm_bwd(d_norm, normed, inv).astype(BF)
        g2_buf[...] = g_two
        yield
        g_one = (mm(w2[...], g_two) * sig * (1.0 + pre * (1.0 - sig))).astype(BF)
        g1_buf[...] = g_one
        yield
        add = mm_t(g_one, hot)
        agg_buf[tile] += add[:, :LANES]
        agg_buf[tile + 1] += add[:, LANES:]

    def weight_sums(item, slot):
        g1_buf, g2_buf, act_buf, hot_buf = slot
        span = pl.ds(pl.multiple_of((item // ITEM_BASE) * SUB, SUB), SUB)
        w2_out[...] += mm_t(act_buf[...], g2_buf[...])
        yield
        w1_out[:latent] += mm_t(he_buf[:, span], g1_buf[...])
        yield
        table_out[...] += mm_t(hot_buf[...], g1_buf[...])

    def together(*parts):
        parts = list(parts)
        while parts:
            for part in list(parts):
                if next(part, parts) is parts:
                    parts.remove(part)

    pairs = jnp.maximum((live_ref[0] + STEP - 1) // STEP, 1)
    per_step = STEP // SUB

    @pl.loop(0, pairs)
    def _(step):
        fit = fit_ref[step] == 1

        @pl.when(fit)
        def _():
            forward_many([step * per_step + sub for sub in range(per_step)], False)

        @pl.when(jnp.logical_not(fit))
        def _():
            @pl.loop(0, per_step)
            def _(sub):
                forward(step * per_step + sub, True)

    node_a, node_b, node_c = slot_a[:3]
    node_a[...] = turned(node_w1[:latent])
    node_b[...] = turned(node_w1[latent:])
    node_c[...] = turned(node_w2[...])
    @pl.loop(0, mesh_tiles // per_sub)
    def _(blk):
        tiles = [blk * per_sub + idx for idx in range(per_sub)]
        hm = jnp.concatenate([hm_t[t] for t in tiles], axis=1)
        agg = jnp.concatenate([agg_buf[t].astype(BF) for t in tiles], axis=1)
        pre = mm(node_a[...], hm) + mm(node_b[...], agg) + col(3, 0)
        sig = sigmoid(pre)
        normed, _, inv = norm_fwd(mm(node_c[...], (pre * sig).astype(BF)) + col(3, 1))
        out = (hm.astype(F32) + (normed * col(3, 2) + col(3, 3))).astype(BF)
        rows = pl.ds(pl.multiple_of(blk * SUB, SUB), SUB)
        mesh_out[rows] = turned(out)
        g_two = norm_bwd(mm_t(eye, cot_ref[rows]) * col(3, 2), normed, inv).astype(BF)
        g_one = (mm(node_w2[...], g_two) * sig * (1.0 + pre * (1.0 - sig))).astype(BF)
        for idx, tile in enumerate(tiles):
            ng_t[tile] = g_one[:, idx * LANES:(idx + 1) * LANES]
    for tile in range(mesh_tiles, ng_t.shape[0]):
        ng_t[tile] = jnp.zeros((latent, LANES), BF)
    agg_buf[...] = jnp.zeros_like(agg_buf)
    for ref in slot_b:
        ref[...] = jnp.zeros_like(ref)

    def list_sub(sub, count):
        def list_tile(step, _):
            item_ref[count + step] = sub * ITEM_BASE + first_ref[sub] + 2 * step
            return 0

        lax.fori_loop(0, span_ref[sub], list_tile, 0)
        return count + span_ref[sub]

    count = lax.fori_loop(0, pairs * per_step, list_sub, 0)
    item_ref[count] = mesh_tiles

    @pl.loop(0, (count + 1) // 2)
    def _(step):
        before, even, odd = item_ref[jnp.maximum(2 * step - 1, 0)], item_ref[2 * step], item_ref[2 * step + 1]
        together(backward(even, slot_a), weight_sums(before, slot_b))
        together(backward(odd, slot_b), weight_sums(even, slot_a))

    together(weight_sums(item_ref[jnp.maximum(2 * ((count + 1) // 2) - 1, 0)], slot_b))

    pieces = split3(table_out[...])
    w1b = w1[latent:2 * latent]
    w1_out[latent:2 * latent] = sum(mm(table_t[...], piece) for piece in pieces)
    table_out[...] = sum(mm_t(piece, w1b) for piece in pieces)
    for blk in range(mesh_tiles // per_sub):
        tiles = range(blk * per_sub, (blk + 1) * per_sub)
        hm = jnp.concatenate([hm_t[t] for t in tiles], axis=1)
        pieces = split3(jnp.concatenate([agg_buf[t] for t in tiles], axis=1))
        part = sum(mm_t(hm, piece) for piece in pieces)
        if blk:
            w1_out[2 * latent:] += part
        else:
            w1_out[2 * latent:] = part


def edge_call(first_tile, spans, fits, live, feats, key_row, mesh_x, below, band, above, small_w, em_w2, mesh_w2, w1, w2,
              node_w1, node_w2, vecs, cot_mesh):
    latent = w2.shape[0]
    edges = key_row.shape[1]
    mesh_rows = cot_mesh.shape[0]
    mesh_tiles = mesh_rows // LANES
    table_rows = below.shape[0] + band.shape[0] + above.shape[0]
    vm = pl.BlockSpec(memory_space=pltpu.VMEM)
    sm = pl.BlockSpec(memory_space=pltpu.SMEM)
    scratch = [((latent, latent), BF), ((latent, 3 * latent), BF), ((latent, latent), BF), ((latent, table_rows), BF),
               ((mesh_tiles, latent, LANES), BF), ((mesh_tiles + 2, latent, LANES), BF), ((8, latent, LANES), F32), ((latent, edges), F32), ((latent, edges), BF),
               ((1, edges), F32), ((1, edges), F32), ((mesh_tiles + 2, latent, LANES), F32)]
    slot = [pltpu.VMEM((latent, SUB), BF)] * 3 + [pltpu.VMEM((table_rows, SUB), BF)]
    items = edges // SUB * (mesh_tiles // 2 + 1) + 2
    return pl.pallas_call(
        edge_kernel,
        in_specs=[sm] * 4 + [vm] * 15, out_specs=[vm] * 4,
        out_shape=[jax.ShapeDtypeStruct((mesh_rows, latent), BF), jax.ShapeDtypeStruct((3 * latent, latent), F32),
                   jax.ShapeDtypeStruct((latent, latent), F32), jax.ShapeDtypeStruct((table_rows, latent), F32)],
        scratch_shapes=[pltpu.VMEM(shape, dtype) for shape, dtype in scratch] + [pltpu.SMEM((items,), jnp.int32)] + slot + slot,
        compiler_params=pltpu.CompilerParams(vmem_limit_bytes=67043328),
        cost_estimate=pl.CostEstimate(flops=36 * edges * latent * latent, bytes_accessed=20 * 2 ** 20,
                                      transcendentals=3 * edges * latent),
        name="edge_both",
    )(first_tile, spans, fits, live, feats, key_row, mesh_x, below, band, above, small_w, em_w2, mesh_w2, w1, w2,
      node_w1, node_w2, vecs, cot_mesh)


STRIDE = {'z': 32, 'y': 8, 'x': 2}
ORDERS = (('x', 'y', 'z'), ('y', 'z', 'x'), ('z', 'x', 'y'))
DIM = 4


def row_norm_bwd(d_norm, normed, inv):
    return inv * (d_norm - jnp.mean(d_norm, axis=1, keepdims=True)
                  - normed * jnp.mean(d_norm * normed, axis=1, keepdims=True))


def finish_kernel(groups, w1_ref, w2_ref, table_ref, band_ref, pre_ref, norm_ref, inv_ref, grid_w1, grid_w2, grid_vec,
                  post_w1, post_w2, post_vec, cot_ref, grid_out, grid_grad, g1_out, g2_out, head_buf, tail_buf, cot_buf,
                  pair1, pair2, *scratch):
    full = scratch[0:3]
    recv = (scratch[3:6], scratch[6:9], scratch[9:12])
    part = (scratch[12:15], scratch[15:18])
    done1, done2, pair_send, pair_recv, hop_send, hop_recv, halo_send, halo_recv = scratch[18:]
    me = lax.axis_index('graph')
    core = me % 2
    coord = {name: (me // stride) % DIM for name, stride in STRIDE.items()}
    partner = me + 1 - 2 * core

    def peer(name, hop):
        there = (coord[name] + hop) % DIM
        return there, me + (there - coord[name]) * STRIDE[name]

    barrier = pltpu.get_barrier_semaphore()
    others = [partner, (me + groups - 1 + 2 * core) % groups]
    others += [peer(name, hop)[1] for name in STRIDE for hop in range(1, DIM)]
    for other in others:
        pl.semaphore_signal(barrier, inc=1, device_id={'graph': other}, device_id_type=MESH)
    pl.semaphore_wait(barrier, len(others))

    half = w1_ref.shape[-1] // 2
    mine = pl.multiple_of(core * half, half)
    theirs = pl.multiple_of((1 - core) * half, half)

    def to_partner(src, dst, slot):
        copy = pltpu.make_async_remote_copy(src_ref=src, dst_ref=dst, send_sem=pair_send.at[slot], recv_sem=pair_recv.at[slot],
                                            device_id={'graph': partner}, device_id_type=MESH)
        copy.start()
        return copy

    first = [to_partner(w1_ref.at[:, :, :, :, pl.ds(theirs, half)], pair1, 0),
             to_partner(w2_ref.at[:, :, :, :, pl.ds(theirs, half)], pair2, 1)]
    halo = head_buf.shape[0]
    rows = band_ref.shape[0]
    halo_copies = []
    for slot, (src, dst, device) in enumerate((
            (table_ref.at[pl.ds(0, halo)], tail_buf, (me + groups - 1) % groups),
            (table_ref.at[pl.ds(halo + rows, halo)], head_buf, (me + 1) % groups))):
        copy = pltpu.make_async_remote_copy(src_ref=src, dst_ref=dst, send_sem=halo_send.at[slot], recv_sem=halo_recv.at[slot],
                                            device_id={'graph': device}, device_id_type=MESH)
        copy.start()
        halo_copies.append(copy)

    band = band_ref[...]
    pre = mm(band, post_w1[...]) + post_vec[0:1]
    sig = sigmoid(pre)
    post_q = mm((pre * sig).astype(BF), post_w2[...]) + post_vec[1:2]
    centred = post_q - jnp.mean(post_q, axis=1, keepdims=True)
    inv = lax.rsqrt(jnp.mean(centred * centred, axis=1, keepdims=True) + NORM_EPS)
    normed = centred * inv
    grid_out[...] = (band.astype(F32) + (normed * post_vec[2:3] + post_vec[3:4])).astype(BF)
    cot = cot_ref[...].astype(F32)
    g_two = row_norm_bwd(cot * post_vec[2:3], normed, inv).astype(BF)
    g_one = (mm_t(g_two, post_w2[...]) * sig * (1.0 + pre * (1.0 - sig))).astype(BF)
    cot_buf[...] = cot + mm_t(g_one, post_w1[...])

    first[0].wait()
    quarter = half // 2
    full[0][...] = w1_ref[:, :, :, :, pl.ds(mine, quarter)] + pair1[:, :, :, :, :quarter]
    full[1][...] = w1_ref[:, :, :, :, pl.ds(mine + quarter, quarter)] + pair1[:, :, :, :, quarter:]
    first[1].wait()
    full[2][...] = w2_ref[:, :, :, :, pl.ds(mine, half)] + pair2[...]

    left = [list(STRIDE) for _ in range(3)]
    held = list(full)

    def at(color, name, index):
        pos = left[color].index(name)
        return (slice(None),) * pos + (index,)

    for stage in range(3):
        copies = []
        for color in range(3):
            name = ORDERS[color][stage]
            for hop in range(1, DIM):
                there, device = peer(name, hop)
                copy = pltpu.make_async_remote_copy(
                    src_ref=held[color].at[at(color, name, there)], dst_ref=recv[stage][color].at[hop - 1],
                    send_sem=hop_send.at[stage, color, hop - 1], recv_sem=hop_recv.at[stage, color, hop - 1],
                    device_id={'graph': device}, device_id_type=MESH)
                copy.start()
                copies.append(copy)
        if stage == 0:
            for copy in halo_copies:
                copy.wait()
            no_halo = jnp.zeros((rows - 2 * halo, head_buf.shape[1]), F32)
            edge_part = table_ref[pl.ds(halo, rows)] + jnp.concatenate(
                [jnp.where(me == 0, 0.0, head_buf[...]), no_halo, jnp.where(me == groups - 1, 0.0, tail_buf[...])], axis=0)
            g_two = row_norm_bwd((cot_buf[...] + edge_part) * grid_vec[2:3], norm_ref[...], inv_ref[...]).astype(BF)
            pre = pre_ref[...]
            sig = sigmoid(pre)
            g_one = (mm_t(g_two, grid_w2[...]) * sig * (1.0 + pre * (1.0 - sig))).astype(BF)
            grid_grad[...] = mm_t(g_one, grid_w1[...])
        for color in range(3):
            for copy in copies[3 * color:3 * color + 3]:
                copy.wait()
            name = ORDERS[color][stage]
            got = recv[stage][color]
            total = held[color][at(color, name, coord[name])] + got[0] + got[1] + got[2]
            left[color].remove(name)
            if stage < 2:
                part[stage][color][...] = total
                held[color] = part[stage][color]
            elif color == 2:
                done2[core] = total
            else:
                done1[core, :, color * quarter:(color + 1) * quarter] = total

    last = [to_partner(done1.at[core], done1.at[core], 2), to_partner(done2.at[core], done2.at[core], 3)]
    for copy in last:
        copy.wait()
    for done, out in ((done1, g1_out), (done2, g2_out)):
        rows = out.shape[0]
        whole = jnp.concatenate([done[0], done[1]], axis=1)
        out[...] = jnp.where(core == 0, whole[:rows], whole[rows:])


def finish_call(groups, w1, w2, table_grad, band, pre, norm, inv, grid_w1, grid_w2, grid_vec, post_w1, post_w2, post_vec, cot):
    rows1, rows2, cols = w1.shape[-2], w2.shape[-2], w1.shape[-1]
    half, quarter = cols // 2, cols // 4
    rows = band.shape[0]
    halo = (table_grad.shape[0] - rows) // 2
    tail = ((rows1, quarter), (rows1, quarter), (rows2, half))
    scratch = [pltpu.VMEM((halo, cols), F32), pltpu.VMEM((halo, cols), F32), pltpu.VMEM((rows, cols), F32)]
    scratch += [pltpu.VMEM((DIM,) * 3 + (rows1, half), F32), pltpu.VMEM((DIM,) * 3 + (rows2, half), F32)]
    scratch += [pltpu.VMEM((DIM,) * 3 + t, F32) for t in tail]
    for stage in range(3):
        scratch += [pltpu.VMEM((3,) + (DIM,) * (2 - stage) + t, F32) for t in tail]
    for stage in range(2):
        scratch += [pltpu.VMEM((DIM,) * (2 - stage) + t, F32) for t in tail]
    scratch += [pltpu.VMEM((2, rows1, half), F32), pltpu.VMEM((2, rows2, half), F32),
                pltpu.SemaphoreType.DMA((4,)), pltpu.SemaphoreType.DMA((4,)),
                pltpu.SemaphoreType.DMA((3, 3, 3)), pltpu.SemaphoreType.DMA((3, 3, 3)),
                pltpu.SemaphoreType.DMA((2,)), pltpu.SemaphoreType.DMA((2,))]
    vm = pl.BlockSpec(memory_space=pltpu.VMEM)
    return pl.pallas_call(
        functools.partial(finish_kernel, groups),
        in_specs=[vm] * 14, out_specs=[vm] * 4,
        out_shape=[jax.ShapeDtypeStruct((rows, cols), BF), jax.ShapeDtypeStruct((rows, grid_w1.shape[0]), F32),
                   jax.ShapeDtypeStruct((rows1 // 2, cols), F32), jax.ShapeDtypeStruct((rows2 // 2, cols), F32)],
        scratch_shapes=scratch,
        compiler_params=pltpu.CompilerParams(collective_id=0, has_side_effects=True, vmem_limit_bytes=67043328),
        name="finish",
    )(w1, w2, table_grad, band, pre, norm, inv, grid_w1, grid_w2, grid_vec, post_w1, post_w2, post_vec, cot)


def mlp_forward(x_in, w_one, w_two, vec_rows):
    pre_one = jnp.dot(x_in, w_one, preferred_element_type=jnp.float32) + vec_rows[0]
    act_bf = jax.nn.silu(pre_one).astype(jnp.bfloat16)
    pre_two = jnp.dot(act_bf, w_two, preferred_element_type=jnp.float32) + vec_rows[1]
    centred = pre_two - jnp.mean(pre_two, axis=-1, keepdims=True)
    inv_std = lax.rsqrt(jnp.mean(centred * centred, axis=-1, keepdims=True) + NORM_EPS)
    normed = centred * inv_std
    return normed * vec_rows[2] + vec_rows[3], (pre_one, act_bf, normed, inv_std)


def solution(mesh):
    groups = mesh.shape['graph']
    row_spec = P(('batch', 'graph'), None)
    flat_spec = P(('batch', 'graph'))
    rep_spec = P(None, None)
    down_perm = [(src_dev, src_dev - 1) for src_dev in range(1, groups)]
    up_perm = [(src_dev, src_dev + 1) for src_dev in range(groups - 1)]

    def device_step(grid_in, mesh_in, edge_in, edge_src, edge_dst, edge_mask, grid_w1, grid_w2, grid_vec,
                    mesh_w1, mesh_w2, mesh_vec, embed_w1, embed_w2, embed_vec, edge_w1, edge_w2, edge_vec,
                    node_w1, node_w2, node_vec, post_w1, post_w2, post_vec, cot_mesh, cot_grid):
        band_rows = grid_in.shape[0]
        halo_rows = band_rows // 4
        latent = grid_w2.shape[1]
        mesh_rows = mesh_in.shape[0]
        edges = edge_in.shape[0]
        mesh_tiles = mesh_rows // LANES
        band_index = lax.axis_index('graph')

        grid_y, grid_saved = mlp_forward(grid_in.astype(BF), grid_w1, grid_w2, grid_vec)
        grid_h = grid_y.astype(BF)
        from_above = lax.ppermute(grid_h[:halo_rows], 'graph', down_perm)
        from_below = lax.ppermute(grid_h[band_rows - halo_rows:], 'graph', up_perm)

        local_src = edge_src - (band_index * band_rows - halo_rows)
        real = edge_mask != 0
        key = jnp.where(real, edge_dst * 2 ** KEY_BITS + local_src, mesh_rows * 2 ** KEY_BITS)
        feat_t = edge_in.T
        key, f0, f1, f2, f3 = lax.sort((key, feat_t[0], feat_t[1], feat_t[2], feat_t[3]), num_keys=1, is_stable=False)
        zero_row = jnp.zeros_like(f0)
        feats = jnp.stack([f0, f1, f2, f3, zero_row, zero_row, zero_row, zero_row])
        live = jnp.sum(real.astype(jnp.int32)).reshape(1)
        dst_sorted = (key >> KEY_BITS).reshape(-1, SUB)
        low = jnp.min(dst_sorted, axis=1)
        high = jnp.max(jnp.where(dst_sorted < mesh_rows, dst_sorted, 0), axis=1)
        first_tile = jnp.minimum(low // LANES, mesh_tiles - 2)
        fits = ((high - first_tile * LANES) < 2 * LANES).reshape(-1, STEP // SUB)
        fits = jnp.all(fits, axis=1).astype(jnp.int32)
        spans = jnp.maximum(high // LANES - first_tile, 0) // 2 + 1
        key_row = key.reshape(1, edges)
        mesh_x = jnp.pad(mesh_in.T, ((0, 8 - mesh_in.shape[1]), (0, 0)))
        small_w = jnp.concatenate([jnp.pad(embed_w1, ((0, 8 - embed_w1.shape[0]), (0, 0))),
                                   jnp.pad(mesh_w1, ((0, 8 - mesh_w1.shape[0]), (0, 0)))])
        vecs = jnp.concatenate([embed_vec, mesh_vec, edge_vec, node_vec])
        mesh_out, w1_part, w2_part, table_grad = edge_call(
            first_tile, spans, fits, live, feats, key_row, mesh_x, from_below, grid_h, from_above, small_w, embed_w2, mesh_w2,
            edge_w1, edge_w2, node_w1, node_w2, vecs, cot_mesh)

        chips = (DIM, DIM, DIM)
        grid_pre, _, grid_norm, grid_inv = grid_saved
        grid_out, grid_grad, w1_grad, w2_grad = finish_call(
            groups, w1_part.reshape(chips + (-1, latent)), w2_part.reshape(chips + (-1, latent)), table_grad, grid_h,
            grid_pre, grid_norm, grid_inv, grid_w1, grid_w2, grid_vec, post_w1, post_w2, post_vec, cot_grid)
        return mesh_out, grid_out, grid_grad, w1_grad, w2_grad

    in_specs = (row_spec, row_spec, row_spec, flat_spec, flat_spec, flat_spec) + (rep_spec,) * 18 + (row_spec, row_spec)
    return jax.shard_map(device_step, mesh=mesh, in_specs=in_specs, out_specs=(row_spec,) * 5, check_vma=False)
```
